32 devices in a mesh: rep: 1 (over z), y: 4 (over y), x: 8 (over x, core).
Axes of the slice: x: 4, y: 4, z: 1, core: 2. Of those that a mesh axis runs over, the one named last changes fastest.
The devices are a block of a 4x4x8 slice.
Arguments:
- hidden: bfloat16 [64, 4096], P('rep', 'y')
- lengths: int32 [64], P('rep')
- k_cache: bfloat16 [2, 64, 128, 32, 128], P(None, ('rep', 'y'), None, 'x')
- v_cache: bfloat16 [2, 64, 128, 32, 128], P(None, ('rep', 'y'), None, 'x')
- rel_table: bfloat16 [2, 128, 32, 128], P(None, None, 'x')
- norm_attn: bfloat16 [2, 4096], P(None, 'y')
- w_q: bfloat16 [2, 4096, 32, 128], P(None, 'y', 'x')
- w_k: bfloat16 [2, 4096, 32, 128], P(None, 'y', 'x')
- w_v: bfloat16 [2, 4096, 32, 128], P(None, 'y', 'x')
- bias_content: bfloat16 [2, 32, 128], P(None, 'x')
- bias_pos: bfloat16 [2, 32, 128], P(None, 'x')
- w_out: bfloat16 [2, 32, 128, 4096], P(None, 'x', None, 'y')
- norm_mlp: bfloat16 [2, 4096], P(None, 'y')
- w_up: bfloat16 [2, 4096, 16384], P(None, 'y', 'x')
- w_down: bfloat16 [2, 16384, 4096], P(None, 'x', 'y')
Outputs:
- output 1: bfloat16 [64, 4096], P('rep', 'y')
- output 2: bfloat16 [2, 64, 128, 32, 128], P(None, ('rep', 'y'), None, 'x')
- output 3: bfloat16 [2, 64, 128, 32, 128], P(None, ('rep', 'y'), None, 'x')
All inputs are finite; a program needn't handle non-finite values.
Results may differ from the reference program's by a relative error of at most 0.02.
Values are sent between devices in bfloat16 or wider.
A program may use at most 768 MiB of HBM per device.

```python
import jax
import jax.numpy as jnp
from jax import lax

D_MODEL = 4096
HEADS = 32
HEAD_DIM = 128
FF_DIM = 16384
SEQ_MAX = 128
BATCH_ROWS = 64
LAYERS = 2

LEN_LOW = max(1, SEQ_MAX // 10)


def relative_table(key):
    feat_half = 64
    dist = jnp.arange(SEQ_MAX, dtype=jnp.float32)
    freqs = 10000.0 ** (-jnp.arange(feat_half, dtype=jnp.float32) / feat_half)
    angle = dist[:, None] * freqs[None, :]
    feats = jnp.concatenate([jnp.sin(angle), jnp.cos(angle)], axis=1)
    proj = jax.random.normal(key, (LAYERS, 2 * feat_half, HEADS * HEAD_DIM), jnp.float32) * feat_half ** -0.5
    table = jnp.einsum("tf,lfe->lte", feats, proj)
    return table.reshape(LAYERS, SEQ_MAX, HEADS, HEAD_DIM).astype(jnp.bfloat16)


def setup_inputs(seed: int = 0, part: int = 0) -> dict:
    base_key = jax.random.key(seed)
    shared = jax.random.split(base_key, 11)
    part_keys = jax.random.split(jax.random.fold_in(base_key, part), 4)

    def normal(key, shape, scale):
        return (jax.random.normal(key, shape, jnp.float32) * scale).astype(jnp.bfloat16)

    def gains(key):
        return (1.0 + 0.3 * jax.random.normal(key, (LAYERS, D_MODEL), jnp.float32)).astype(jnp.bfloat16)

    model_scale = D_MODEL ** -0.5
    out_scale = (HEADS * HEAD_DIM) ** -0.5 * (SEQ_MAX / 64) ** 0.5
    proj_shape = (LAYERS, D_MODEL, HEADS, HEAD_DIM)
    cache_shape = (LAYERS, BATCH_ROWS, SEQ_MAX, HEADS, HEAD_DIM)
    lengths = jax.random.randint(part_keys[3], (BATCH_ROWS,), LEN_LOW, SEQ_MAX, dtype=jnp.int32)
    lengths = lengths.at[0].set(SEQ_MAX - 1).at[1].set(LEN_LOW)
    return {
        "hidden": normal(part_keys[0], (BATCH_ROWS, D_MODEL), 1.0),
        "lengths": lengths,
        "k_cache": normal(part_keys[1], cache_shape, 1.0),
        "v_cache": normal(part_keys[2], cache_shape, 1.0),
        "rel_table": relative_table(shared[0]),
        "norm_attn": gains(shared[1]),
        "w_q": normal(shared[2], proj_shape, model_scale),
        "w_k": normal(shared[3], proj_shape, model_scale),
        "w_v": normal(shared[4], proj_shape, model_scale),
        "bias_content": normal(shared[5], (LAYERS, HEADS, HEAD_DIM), 0.5),
        "bias_pos": normal(shared[6], (LAYERS, HEADS, HEAD_DIM), 0.5),
        "w_out": normal(shared[7], (LAYERS, HEADS, HEAD_DIM, D_MODEL), out_scale),
        "norm_mlp": gains(shared[8]),
        "w_up": normal(shared[9], (LAYERS, D_MODEL, FF_DIM), model_scale),
        "w_down": normal(shared[10], (LAYERS, FF_DIM, D_MODEL), FF_DIM ** -0.5),
    }


def rms_norm(values, gain):
    wide = values.astype(jnp.float32)
    inv_rms = lax.rsqrt(jnp.mean(wide * wide, axis=-1, keepdims=True) + 1e-6)
    return (wide * inv_rms * gain.astype(jnp.float32)).astype(jnp.bfloat16)


def project(normed, weight):
    flat = jnp.dot(normed, weight.reshape(D_MODEL, HEADS * HEAD_DIM), preferred_element_type=jnp.float32)
    return flat.reshape(BATCH_ROWS, HEADS, HEAD_DIM).astype(jnp.bfloat16)


def reference(hidden, lengths, k_cache, v_cache, rel_table, norm_attn, w_q, w_k, w_v, bias_content, bias_pos, w_out, norm_mlp, w_up, w_down):
    positions = jnp.arange(SEQ_MAX)
    row_ids = jnp.arange(BATCH_ROWS)

    def layer_step(state, layer_args):
        (k_layer, v_layer, rel_layer, gain_attn, wq_layer, wk_layer, wv_layer,
         content_bias, pos_bias, wout_layer, gain_mlp, wup_layer, wdown_layer) = layer_args
        normed = rms_norm(state, gain_attn)
        q_new = project(normed, wq_layer)
        k_new = project(normed, wk_layer)
        v_new = project(normed, wv_layer)
        k_upd = k_layer.at[row_ids, lengths].set(k_new)
        v_upd = v_layer.at[row_ids, lengths].set(v_new)
        rel_wide = rel_layer.astype(jnp.float32)
        cbias_wide = content_bias.astype(jnp.float32)
        pbias_wide = pos_bias.astype(jnp.float32)

        def attend_row(row_args):
            q_row, k_rows, v_rows, length = row_args
            q_wide = q_row.astype(jnp.float32)
            q_content = (q_wide + cbias_wide).astype(jnp.bfloat16).astype(jnp.float32)
            q_pos = (q_wide + pbias_wide).astype(jnp.bfloat16).astype(jnp.float32)
            rel_rows = jnp.take(rel_wide, jnp.maximum(length - positions, 0), axis=0)
            scores = jnp.einsum("he,she->hs", q_content, k_rows.astype(jnp.float32))
            scores = scores + jnp.einsum("he,she->hs", q_pos, rel_rows)
            scores = jnp.where(positions[None, :] <= length, scores * HEAD_DIM ** -0.5, -1e30)
            attn_prob = jax.nn.softmax(scores, axis=-1).astype(jnp.bfloat16).astype(jnp.float32)
            return jnp.einsum("hs,she->he", attn_prob, v_rows.astype(jnp.float32)).astype(jnp.bfloat16)

        context = lax.map(attend_row, (q_new, k_upd, v_upd, lengths))
        attn_out = jnp.dot(context.reshape(BATCH_ROWS, HEADS * HEAD_DIM), wout_layer.reshape(HEADS * HEAD_DIM, D_MODEL), preferred_element_type=jnp.float32)
        state = (state.astype(jnp.float32) + attn_out).astype(jnp.bfloat16)
        normed = rms_norm(state, gain_mlp)
        up_proj = jnp.dot(normed, wup_layer, preferred_element_type=jnp.float32).astype(jnp.bfloat16)
        activated = jax.nn.gelu(up_proj.astype(jnp.float32), approximate=True).astype(jnp.bfloat16)
        down_out = jnp.dot(activated, wdown_layer, preferred_element_type=jnp.float32)
        state = (state.astype(jnp.float32) + down_out).astype(jnp.bfloat16)
        return state, (k_upd, v_upd)

    final, (k_all, v_all) = lax.scan(layer_step, hidden, (k_cache, v_cache, rel_table, norm_attn, w_q, w_k, w_v, bias_content, bias_pos, w_out, norm_mlp, w_up, w_down))
    return final, k_all, v_all
```

```python
import functools

import jax
import jax.numpy as jnp
from jax import lax
from jax.experimental import pallas as pl
from jax.experimental.pallas import tpu as pltpu
from jax.sharding import PartitionSpec as P

EPS = 1e-6
F32 = jnp.float32
BF16 = jnp.bfloat16
MESH = pl.DeviceIdType.MESH


def step_kernel(dims, hidden_in, len_in, kc_in, vc_in, rel_in, na_in, wq_in, wk_in, wv_in, bu_in, bw_in, wo_in, nm_in, wup_in, wdn_in,
                hid_out, kn_out, vn_out,
                hid_v, len_v, kc_v, vc_v, rel_v, na_v, nm_v, bu_v, bw_v, wraw_v, wqkv_v, wo_v, wup_v, wdn_v,
                wtmp, relf_v, r0_v, h_v, a_s, c_s, k_s, v_s, ctx_s, kn_v, vn_v, acc_v, outh_v,
                ss_rx, qkv_tx, qkv_rx, ctx_all, rs_tx, rs_rx, xg, up_tx, up_rx, act,
                ld_sem, out_sem, ss_ss, ss_rs, qkv_ss, qkv_rs, ctx_ss, ctx_rs, rs_ss, rs_rs, ag_ss, ag_rs, up_ss, up_rs, act_ss, act_rs):
    layers, ny, nx, rows, heads, hd, seq, d_loc, ff_loc = dims
    d_total = d_loc * ny
    rb = rows // ny
    hh = heads * hd
    cb = d_loc // nx
    fb = ff_loc // ny
    cells = rb * heads
    kl = seq * heads
    chips = nx // 2
    my = lax.axis_index("y")
    mx = lax.axis_index("x")
    my_chip = mx // 2
    my_core = lax.rem(mx, 2)
    partner = 2 * my_chip + 1 - my_core

    barrier = pltpu.get_barrier_semaphore()
    for d in range(1, ny):
        pl.semaphore_signal(barrier, inc=1, device_id={"y": lax.rem(my + d, ny)}, device_id_type=MESH)
    for d in range(1, nx):
        pl.semaphore_signal(barrier, inc=1, device_id={"x": lax.rem(mx + d, nx)}, device_id_type=MESH)

    loads = {}

    def load(name, src, dst):
        c = pltpu.make_async_copy(src, dst, ld_sem.at[len(loads)])
        c.start()
        loads[name] = c

    load("hid", hidden_in, hid_v)
    load("na", na_in, na_v)
    for j, w in enumerate((wq_in, wk_in, wv_in)):
        load(("w", 0, j), w.at[0], wraw_v.at[0, j])
    load("len", len_in, len_v)
    load("rel", rel_in, rel_v)
    load("bu", bu_in, bu_v)
    load("bw", bw_in, bw_v)
    load("nm", nm_in, nm_v)
    load(("k", 0), kc_in.at[0], kc_v.at[0])
    load(("v", 0), vc_in.at[0], vc_v.at[0])
    load(("o", 0), wo_in.at[0], wo_v.at[0])
    load(("up", 0), wup_in.at[0], wup_v.at[0])
    load(("dn", 0), wdn_in.at[0], wdn_v.at[0])
    for l in range(1, layers):
        for j, w in enumerate((wq_in, wk_in, wv_in)):
            load(("w", l, j), w.at[l], wraw_v.at[l, j])
        load(("k", l), kc_in.at[l], kc_v.at[l])
        load(("v", l), vc_in.at[l], vc_v.at[l])
        load(("o", l), wo_in.at[l], wo_v.at[l])
        load(("up", l), wup_in.at[l], wup_v.at[l])
        load(("dn", l), wdn_in.at[l], wdn_v.at[l])

    sends = []

    def send(src, dst, ss, rs, dev):
        c = pltpu.make_async_remote_copy(src_ref=src, dst_ref=dst, send_sem=ss, recv_sem=rs, device_id=dev, device_id_type=MESH)
        c.start()
        sends.append(c)

    def recv(dst, ss, rs, dev):
        pltpu.make_async_remote_copy(src_ref=dst, dst_ref=dst, send_sem=ss, recv_sem=rs, device_id=dev, device_id_type=MESH).wait_recv()

    y_order = [2, 1, 3] if ny == 4 else list(range(1, ny))
    chunk_k = 128
    chunk = chunk_k * heads

    def relayout(l, j):
        def body(i, carry):
            wtmp[...] = wraw_v[l, j, pl.ds(pl.multiple_of(i * chunk, chunk), chunk), :].astype(F32)
            for h in range(heads):
                wqkv_v[l, pl.ds(pl.multiple_of(i * chunk_k, chunk_k), chunk_k), j * hh + h * hd:j * hh + (h + 1) * hd] = wtmp[pl.ds(h, chunk_k, stride=heads), :].astype(BF16)
            return carry
        lax.fori_loop(0, d_loc // chunk_k, body, 0)

    lane = lax.broadcasted_iota(jnp.int32, (rows, 128), 1)
    rown = lax.broadcasted_iota(jnp.int32, (rows, 128), 0)
    diag = lane == rown

    def norm_stage(n, p, gain):
        blocks = [xg[p, j].astype(F32) for j in range(nx)]
        sq = blocks[0] * blocks[0]
        for j in range(1, nx):
            sq = sq + blocks[j] * blocks[j]
        ssq = jnp.sum(sq, axis=1, keepdims=True)
        row = jnp.sum(jnp.where(diag, ssq, 0.0), axis=0, keepdims=True)
        ss_rx[n, my] = jnp.broadcast_to(row, (8, 128))
        for d in y_order:
            peer = lax.rem(my + d, ny)
            send(ss_rx.at[n, my], ss_rx.at[n, my], ss_ss.at[n, peer], ss_rs.at[n, my], {"y": peer})
        inv = lax.rsqrt(ssq / d_loc + EPS)
        for j in range(nx):
            h_v[:, j * cb:(j + 1) * cb] = (blocks[j] * inv * gain[:, j * cb:(j + 1) * cb].astype(F32)).astype(BF16)

    def ratio_rows(n):
        for d in y_order:
            src = lax.rem(my + d, ny)
            recv(ss_rx.at[n, src], ss_ss.at[n, src], ss_rs.at[n, src], {"y": src})
        parts = [ss_rx[n, s][0:1] for s in range(ny)]
        total = parts[0]
        for s in range(1, ny):
            total = total + parts[s]
        inv = lax.rsqrt(total / d_total + EPS)
        finite = total < jnp.inf
        return [jnp.where(finite, inv * jnp.sqrt(parts[s] / d_loc + EPS), 0.0) for s in range(ny)]

    def to_column(row, index):
        return jnp.sum(jnp.where(lax.broadcasted_iota(jnp.int32, index.shape, 1) == index, row, 0.0), axis=1, keepdims=True)

    def x_reduce(p, matmul):
        for dc in ([2, 1, 3, 0] if chips == 4 else list(range(1, chips)) + [0]):
            chip = lax.rem(my_chip + dc, chips)
            part = matmul(pl.multiple_of(chip * 2 * cb, 2 * cb)).astype(BF16)
            rs_tx[p, 2 * chip] = part[:, :cb]
            rs_tx[p, 2 * chip + 1] = part[:, cb:]
            if dc:
                for core in range(2):
                    dst = 2 * chip + core
                    send(rs_tx.at[p, dst], rs_rx.at[p, mx], rs_ss.at[p, dst], rs_rs.at[p, mx], {"x": dst})
            else:
                send(rs_tx.at[p, partner], rs_rx.at[p, mx], rs_ss.at[p, partner], rs_rs.at[p, mx], {"x": partner})
        total = rs_tx[p, mx].astype(F32)
        for d in [nx - d for d in range(1, nx)]:
            src = lax.rem(mx + d, nx)
            recv(rs_rx.at[p, src], rs_ss.at[p, src], rs_rs.at[p, src], {"x": src})
            total = total + rs_rx[p, src].astype(F32)
        xg[p + 1, mx] = (xg[p, mx].astype(F32) + total).astype(BF16)
        for d in [4, 3, 5, 2, 6, 1, 7]:
            dst = lax.rem(mx + d, nx)
            send(xg.at[p + 1, mx], xg.at[p + 1, mx], ag_ss.at[p, dst], ag_rs.at[p, mx], {"x": dst})

    def x_gather_wait(p):
        for d in range(1, nx):
            src = lax.rem(mx + d, nx)
            recv(xg.at[p + 1, src], ag_ss.at[p, src], ag_rs.at[p, src], {"x": src})

    loads["hid"].wait()
    for j in range(nx):
        xg[0, j] = hid_v[:, j * cb:(j + 1) * cb]
    for j in range(3):
        loads["w", 0, j].wait()
        relayout(0, j)
    loads["na"].wait()
    loads["len"].wait()
    loads["rel"].wait()
    loads["bu"].wait()
    loads["bw"].wait()
    loads["nm"].wait()
    pl.semaphore_wait(barrier, ny - 1 + nx - 1)

    cell_row = lax.broadcasted_iota(jnp.int32, (cells, 1), 0)
    key_lane = lax.broadcasted_iota(jnp.int32, (cells, kl), 1)
    key_row = lax.broadcasted_iota(jnp.int32, (cells, kl), 0)
    group_row = lax.broadcasted_iota(jnp.int32, (16, 1), 0) // heads
    per_group = 16 // heads

    def prepare_rel(l):
        pr = lax.broadcasted_iota(jnp.int32, (kl, kl), 0)
        pc = lax.broadcasted_iota(jnp.int32, (kl, kl), 1)
        flip = (pc == (seq - 1 - pr // heads) * heads + lax.rem(pr, heads)).astype(F32).astype(BF16)
        relf_v[l] = jnp.dot(flip, rel_v[l], preferred_element_type=F32).astype(BF16)
        first = rel_v[l, 0:16].astype(F32)
        for h in range(heads):
            r0_v[l, pl.ds(h, rb, stride=heads), :] = jnp.broadcast_to(first[h:h + 1], (rb, hd))

    for l in range(layers):
        p = 2 * l
        norm_stage(2 * l, p, na_v[l:l + 1])
        for j in range(3):
            part = jnp.dot(h_v[...], wqkv_v[l, :, j * hh:(j + 1) * hh], preferred_element_type=F32)
            qkv_tx[l, j] = part.astype(BF16)
            for d in y_order:
                peer = lax.rem(my + d, ny)
                rows_at = pl.multiple_of(peer * rb, rb)
                send(qkv_tx.at[l, j, pl.ds(rows_at, rb)], qkv_rx.at[l, my, j], qkv_ss.at[l, j, peer], qkv_rs.at[l, j, my], {"y": peer})
        own_at = pl.multiple_of(my * rb, rb)
        for j in range(3):
            qkv_rx[l, my, j] = qkv_tx[l, j, pl.ds(own_at, rb), :]
        if l == 0:
            for l2 in range(layers):
                prepare_rel(l2)
            for l2 in range(1, layers):
                for j in range(3):
                    loads["w", l2, j].wait()
                    relayout(l2, j)
        lens_row = len_v[...].astype(F32)
        want = my * rb + lax.broadcasted_iota(jnp.int32, (cells, rows), 0) // heads
        lens = to_column(lens_row, want).astype(jnp.int32)
        ratios = ratio_rows(2 * l)
        want16 = my * rb + lax.broadcasted_iota(jnp.int32, (rb, 128), 0)
        cols = [to_column(r, want16) for r in ratios]

        def gathered(j):
            for d in y_order:
                src = lax.rem(my + d, ny)
                recv(qkv_rx.at[l, src, j], qkv_ss.at[l, j, src], qkv_rs.at[l, j, src], {"y": src})
            tot = qkv_rx[l, 0, j].astype(F32) * cols[0]
            for s in range(1, ny):
                tot = tot + qkv_rx[l, s, j].astype(F32) * cols[s]
            return tot.astype(BF16).astype(F32)

        q = gathered(0)
        for h in range(heads):
            qh = q[:, h * hd:(h + 1) * hd]
            a_s[pl.ds(h, rb, stride=heads), :] = qh + bu_v[l, h:h + 1].astype(F32)
            c_s[pl.ds(h, rb, stride=heads), :] = qh + bw_v[l, h:h + 1].astype(F32)
        a = a_s[...].astype(BF16)
        c = c_s[...].astype(BF16)
        rel = lax.dot_general(c, relf_v[l], (((1,), (1,)), ((), ())), preferred_element_type=F32)
        shift = seq - 1 - lens
        bit = 1
        while bit < seq:
            rolled = pltpu.roll(rel, kl - bit * heads, 1)
            rel = jnp.where(lax.rem(shift // bit, 2) == 1, rolled, rel)
            bit *= 2
        loads["k", l].wait()
        score_parts = []
        for g in range(cells // 16):
            ag = a[16 * g:16 * g + 16]
            sg = None
            for i in range(per_group):
                o = lax.dot_general(ag, kc_v[l, g * per_group + i], (((1,), (1,)), ((), ())), preferred_element_type=F32)
                sg = o if sg is None else jnp.where(group_row == i, o, sg)
            score_parts.append(sg)
        scores = jnp.concatenate(score_parts, axis=0)
        k = gathered(1)
        v = gathered(2)
        for h in range(heads):
            k_s[pl.ds(h, rb, stride=heads), :] = k[:, h * hd:(h + 1) * hd]
            v_s[pl.ds(h, rb, stride=heads), :] = v[:, h * hd:(h + 1) * hd]
        kn = k_s[...]
        vn = v_s[...]
        kn_v[l] = kn.astype(BF16)
        vn_v[l] = vn.astype(BF16)
        scale = hd ** -0.5
        s_new = (jnp.sum(a.astype(F32) * kn, axis=1, keepdims=True) + jnp.sum(c.astype(F32) * r0_v[l], axis=1, keepdims=True)) * scale
        valid = (lax.rem(key_lane, heads) == lax.rem(key_row, heads)) & (key_lane // heads < lens)
        scores = jnp.where(valid, (scores + rel) * scale, -jnp.inf)
        top = jnp.maximum(jnp.max(scores, axis=1, keepdims=True), s_new)
        e = jnp.exp(scores - top)
        e_new = jnp.exp(s_new - top)
        inv_den = 1.0 / (jnp.sum(e, axis=1, keepdims=True) + e_new)
        prob = (e * inv_den).astype(BF16)
        p_new = (e_new * inv_den).astype(BF16).astype(F32)
        loads["v", l].wait()
        ctx_parts = []
        for g in range(cells // 16):
            pg = prob[16 * g:16 * g + 16]
            cg = None
            for i in range(0, per_group, 2):
                b = g * per_group + i
                pair = jnp.concatenate([vc_v[l, b], vc_v[l, b + 1]], axis=1)
                o = jnp.dot(pg, pair, preferred_element_type=F32)
                cg = o[:, :hd] if cg is None else jnp.where(group_row == i, o[:, :hd], cg)
                cg = jnp.where(group_row == i + 1, o[:, hd:], cg)
            ctx_parts.append(cg)
        ctx_s[...] = jnp.concatenate(ctx_parts, axis=0) + p_new * vn
        for h in range(heads):
            ctx_all[l, my, :, h * hd:(h + 1) * hd] = ctx_s[pl.ds(h, rb, stride=heads), :].astype(BF16)
        for d in y_order:
            peer = lax.rem(my + d, ny)
            send(ctx_all.at[l, my], ctx_all.at[l, my], ctx_ss.at[l, peer], ctx_rs.at[l, my], {"y": peer})
        loads["o", l].wait()
        for d in y_order:
            src = lax.rem(my + d, ny)
            recv(ctx_all.at[l, src], ctx_ss.at[l, src], ctx_rs.at[l, src], {"y": src})
        ctx = jnp.concatenate([ctx_all[l, s] for s in range(ny)], axis=0)
        x_reduce(p, lambda at: jnp.dot(ctx, wo_v[l, :, pl.ds(at, 2 * cb)], preferred_element_type=F32))
        x_gather_wait(p)
        p = 2 * l + 1
        norm_stage(p, p, nm_v[l:l + 1])
        loads["up", l].wait()
        for d in y_order + [0]:
            dst = lax.rem(my + d, ny)
            part = jnp.dot(h_v[...], wup_v[l, :, pl.ds(pl.multiple_of(dst * fb, fb), fb)], preferred_element_type=F32).astype(BF16)
            if d:
                up_tx[l, dst] = part
                send(up_tx.at[l, dst], up_rx.at[l, my], up_ss.at[l, dst], up_rs.at[l, my], {"y": dst})
            else:
                up_rx[l, my] = part
        ratios = ratio_rows(p)
        cols = [to_column(r, rown) for r in ratios]
        for d in y_order:
            src = lax.rem(my + d, ny)
            recv(up_rx.at[l, src], up_ss.at[l, src], up_rs.at[l, src], {"y": src})
        tot = up_rx[l, 0].astype(F32) * cols[0]
        for s in range(1, ny):
            tot = tot + up_rx[l, s].astype(F32) * cols[s]
        act[l, my] = jax.nn.gelu(tot.astype(BF16).astype(F32), approximate=True).astype(BF16)
        for d in y_order:
            peer = lax.rem(my + d, ny)
            send(act.at[l, my], act.at[l, my], act_ss.at[l, peer], act_rs.at[l, my], {"y": peer})
        loads["dn", l].wait()

        def down_rows(src):
            return pl.ds(pl.multiple_of(src * fb, fb), fb)

        acc_v[...] = jnp.dot(act[l, my], wdn_v[l, down_rows(my), :], preferred_element_type=F32)
        for d in reversed(y_order[1:]):
            src = lax.rem(my + d, ny)
            recv(act.at[l, src], act_ss.at[l, src], act_rs.at[l, src], {"y": src})
            acc_v[...] += jnp.dot(act[l, src], wdn_v[l, down_rows(src), :], preferred_element_type=F32)
        src = lax.rem(my + y_order[0], ny)
        recv(act.at[l, src], act_ss.at[l, src], act_rs.at[l, src], {"y": src})
        x_reduce(p, lambda at: acc_v[:, pl.ds(at, 2 * cb)] + jnp.dot(act[l, src], wdn_v[l, down_rows(src), pl.ds(at, 2 * cb)], preferred_element_type=F32))
        x_gather_wait(p)

    last = 2 * layers
    for j in range(nx):
        outh_v[:, j * cb:(j + 1) * cb] = xg[last, j]
    outs = [pltpu.make_async_copy(outh_v, hid_out, out_sem.at[0]),
            pltpu.make_async_copy(kn_v, kn_out, out_sem.at[1]),
            pltpu.make_async_copy(vn_v, vn_out, out_sem.at[2])]
    for o in outs:
        o.start()
    for c in sends:
        c.wait_send()
    for o in outs:
        o.wait()


def cache_kernel(dims, len_ref, hid_in, kc_in, vc_in, kn_in, vn_in, hid_out, kc_out, vc_out, hid_v, kc_v, vc_v, kn_v, vn_v, in_sem, out_sem):
    layers, rb = dims
    my = lax.axis_index("y")
    ins = []
    for i, (src, dst) in enumerate(((kn_in, kn_v), (vn_in, vn_v), (hid_in, hid_v))):
        c = pltpu.make_async_copy(src, dst, in_sem.at[i])
        c.start()
        ins.append(c)
    half = rb // 2
    parts = []
    for l in range(layers):
        for src, buf, new, dst in ((kc_in, kc_v, kn_v, kc_out), (vc_in, vc_v, vn_v, vc_out)):
            for s in range(2):
                at = pl.ds(s * half, half)
                i = len(parts)
                r = pltpu.make_async_copy(src.at[l, at], buf.at[l, at], in_sem.at[3 + i])
                r.start()
                parts.append((r, pltpu.make_async_copy(buf.at[l, at], dst.at[l, at], out_sem.at[1 + i]), buf, new, l, s * half))
    for c in ins:
        c.wait()
    out_h = pltpu.make_async_copy(hid_v, hid_out, out_sem.at[0])
    out_h.start()
    for r, w, buf, new, l, b0 in parts:
        r.wait()
        for b in range(b0, b0 + half):
            buf[l, b, len_ref[my * rb + b]] = new[l, b]
        w.start()
    out_h.wait()
    for part in parts:
        part[1].wait()


def solution(mesh):
    ny = mesh.shape["y"]
    nx = mesh.shape["x"]
    cache_spec = P(None, ("rep", "y"), None, "x", None)
    row_spec = P("rep", "y")
    proj_spec = P(None, "y", "x", None)
    head_spec = P(None, "x", None)
    in_specs = (row_spec, P("rep"), cache_spec, cache_spec, P(None, None, "x", None), P(None, "y"),
                proj_spec, proj_spec, proj_spec, head_spec, head_spec, P(None, "x", None, "y"),
                P(None, "y"), P(None, "y", "x"), P(None, "x", "y"))
    out_specs = (row_spec, cache_spec, cache_spec)

    def local_step(hidden, lengths, k_cache, v_cache, rel_table, norm_attn, w_q, w_k, w_v, bias_content, bias_pos, w_out, norm_mlp, w_up, w_down):
        layers, rb, seq, heads, hd = k_cache.shape
        rows, d_loc = hidden.shape
        ff_loc = w_up.shape[2]
        hh = heads * hd
        cells = rb * heads
        kl = seq * heads
        cb = d_loc // nx
        fb = ff_loc // ny
        dims = (layers, ny, nx, rows, heads, hd, seq, d_loc, ff_loc)
        any_spec = pl.BlockSpec(memory_space=pl.ANY)
        vmem = pltpu.VMEM
        dma = pltpu.SemaphoreType.DMA
        scratch = [
            vmem((rows, d_loc), BF16), vmem((1, rows), jnp.int32),
            vmem((layers, rb, kl, hd), BF16), vmem((layers, rb, kl, hd), BF16),
            vmem((layers, kl, hd), BF16), vmem((layers, d_loc), BF16), vmem((layers, d_loc), BF16),
            vmem((layers, heads, hd), BF16), vmem((layers, heads, hd), BF16),
            vmem((layers, 3, d_loc * heads, hd), BF16), vmem((layers, d_loc, 3 * hh), BF16),
            vmem((layers, hh, d_loc), BF16), vmem((layers, d_loc, ff_loc), BF16), vmem((layers, ff_loc, d_loc), BF16),
            vmem((128 * heads, hd), F32), vmem((layers, kl, hd), BF16), vmem((layers, cells, hd), F32), vmem((rows, d_loc), BF16),
            vmem((cells, hd), F32), vmem((cells, hd), F32), vmem((cells, hd), F32), vmem((cells, hd), F32), vmem((cells, hd), F32),
            vmem((layers, cells, hd), BF16), vmem((layers, cells, hd), BF16), vmem((rows, d_loc), F32), vmem((rows, d_loc), BF16),
            vmem((2 * layers, ny, 8, 128), F32),
            vmem((layers, 3, rows, hh), BF16), vmem((layers, ny, 3, rb, hh), BF16), vmem((layers, ny, rb, hh), BF16),
            vmem((2 * layers, nx, rows, cb), BF16), vmem((2 * layers, nx, rows, cb), BF16), vmem((2 * layers + 1, nx, rows, cb), BF16),
            vmem((layers, ny, rows, fb), BF16), vmem((layers, ny, rows, fb), BF16), vmem((layers, ny, rows, fb), BF16),
            dma((7 + 8 * layers,)), dma((3,)),
            dma((2 * layers, ny)), dma((2 * layers, ny)), dma((layers, 3, ny)), dma((layers, 3, ny)),
            dma((layers, ny)), dma((layers, ny)), dma((2 * layers, nx)), dma((2 * layers, nx)),
            dma((2 * layers, nx)), dma((2 * layers, nx)), dma((layers, ny)), dma((layers, ny)), dma((layers, ny)), dma((layers, ny)),
        ]
        new_shape = jax.ShapeDtypeStruct((layers, cells, hd), BF16)
        hid, k_new, v_new = pl.pallas_call(
            functools.partial(step_kernel, dims),
            out_shape=(jax.ShapeDtypeStruct((rows, d_loc), BF16), new_shape, new_shape),
            in_specs=[any_spec] * 15,
            out_specs=(any_spec,) * 3,
            scratch_shapes=scratch,
            compiler_params=pltpu.CompilerParams(collective_id=0, has_side_effects=True, vmem_limit_bytes=67043328),
            name="decode_step",
        )(hidden, lengths.reshape(1, rows), k_cache.reshape(layers, rb, kl, hd), v_cache.reshape(layers, rb, kl, hd),
          rel_table.reshape(layers, kl, hd), norm_attn,
          w_q.reshape(layers, d_loc * heads, hd), w_k.reshape(layers, d_loc * heads, hd), w_v.reshape(layers, d_loc * heads, hd),
          bias_content, bias_pos, w_out.reshape(layers, hh, d_loc), norm_mlp, w_up, w_down)

        cache_shape = jax.ShapeDtypeStruct(k_cache.shape, BF16)
        return pl.pallas_call(
            functools.partial(cache_kernel, (layers, rb)),
            out_shape=(jax.ShapeDtypeStruct((rows, d_loc), BF16), cache_shape, cache_shape),
            in_specs=[pl.BlockSpec(memory_space=pltpu.SMEM)] + [any_spec] * 5,
            out_specs=(any_spec,) * 3,
            scratch_shapes=[
                vmem((rows, d_loc), BF16), vmem(k_cache.shape, BF16), vmem(k_cache.shape, BF16),
                vmem((layers, rb, heads, hd), BF16), vmem((layers, rb, heads, hd), BF16),
                dma((3 + 4 * layers,)), dma((1 + 4 * layers,)),
            ],
            name="cache_write",
        )(lengths, hid, k_cache, v_cache, k_new.reshape(layers, rb, heads, hd), v_new.reshape(layers, rb, heads, hd))

    return jax.shard_map(local_step, mesh=mesh, in_specs=in_specs, out_specs=out_specs, check_vma=False)
```

```python
import functools

import jax
import jax.numpy as jnp
from jax import lax
from jax.experimental import pallas as pl
from jax.experimental.pallas import tpu as pltpu
from jax.sharding import PartitionSpec as P

EPS = 1e-6
F32 = jnp.float32
BF16 = jnp.bfloat16
MESH = pl.DeviceIdType.MESH


def step_kernel(dims, hidden_in, len_in, kc_in, vc_in, rel_in, na_in, wq_in, wk_in, wv_in, bu_in, bw_in, wo_in, nm_in, wup_in, wdn_in,
                hid_out, kc_v, vc_v,
                hid_v, len_v, rel_v, na_v, nm_v, bu_v, bw_v, wraw_v, wqkv_v, wo_v, wup_v, wdn_v,
                wtmp, relf_v, r0_v, h_v, a_s, c_s, k_s, v_s, ctx_s, acc_v, pos_v, lent_s, kt_s, vt_s,
                ss_rx, qkv_tx, qkv_rx, ctx_all, rs_tx, rs_rx, xg, up_tx, up_rx, act,
                ld_sem, ss_ss, ss_rs, qkv_ss, qkv_rs, ctx_ss, ctx_rs, rs_ss, rs_rs, ag_ss, ag_rs, up_ss, up_rs, act_ss, act_rs):
    layers, ny, nx, rows, heads, hd, seq, d_loc, ff_loc = dims
    d_total = d_loc * ny
    rb = rows // ny
    hh = heads * hd
    cb = d_loc // nx
    fb = ff_loc // ny
    cells = rb * heads
    kl = seq * heads
    my = lax.axis_index("y")
    mx = lax.axis_index("x")

    barrier = pltpu.get_barrier_semaphore()
    for d in range(1, ny):
        pl.semaphore_signal(barrier, inc=1, device_id={"y": lax.rem(my + d, ny)}, device_id_type=MESH)
    for d in range(1, nx):
        pl.semaphore_signal(barrier, inc=1, device_id={"x": lax.rem(mx + d, nx)}, device_id_type=MESH)

    loads = {}

    def load(name, src, dst):
        c = pltpu.make_async_copy(src, dst, ld_sem.at[len(loads)])
        c.start()
        loads[name] = c

    load("hid", hidden_in, hid_v)
    load("na", na_in, na_v)
    for j, w in enumerate((wq_in, wk_in, wv_in)):
        load(("w", 0, j), w.at[0], wraw_v.at[0, j])
    load("len", len_in, len_v)
    load("rel", rel_in, rel_v)
    load("bu", bu_in, bu_v)
    load("bw", bw_in, bw_v)
    load("nm", nm_in, nm_v)
    load(("k", 0), kc_in.at[0], kc_v.at[0])
    load(("v", 0), vc_in.at[0], vc_v.at[0])
    load(("o", 0), wo_in.at[0], wo_v.at[0])
    load(("up", 0), wup_in.at[0], wup_v.at[0])
    load(("dn", 0), wdn_in.at[0], wdn_v.at[0])
    for l in range(1, layers):
        for j, w in enumerate((wq_in, wk_in, wv_in)):
            load(("w", l, j), w.at[l], wraw_v.at[l, j])
        load(("k", l), kc_in.at[l], kc_v.at[l])
        load(("v", l), vc_in.at[l], vc_v.at[l])
        load(("o", l), wo_in.at[l], wo_v.at[l])
        load(("up", l), wup_in.at[l], wup_v.at[l])
        load(("dn", l), wdn_in.at[l], wdn_v.at[l])

    sends = []

    def send(src, dst, ss, rs, dev):
        c = pltpu.make_async_remote_copy(src_ref=src, dst_ref=dst, send_sem=ss, recv_sem=rs, device_id=dev, device_id_type=MESH)
        c.start()
        sends.append(c)

    def recv(dst, ss, rs, dev):
        pltpu.make_async_remote_copy(src_ref=dst, dst_ref=dst, send_sem=ss, recv_sem=rs, device_id=dev, device_id_type=MESH).wait_recv()

    x_order = sorted(range(1, nx), key=lambda d: -min(d, nx - d))
    y_order = [2, 1, 3] if ny == 4 else list(range(1, ny))
    chunk_k = 128
    chunk = chunk_k * heads

    def relayout(l, j):
        def body(i, carry):
            wtmp[...] = wraw_v[l, j, pl.ds(pl.multiple_of(i * chunk, chunk), chunk), :].astype(F32)
            for h in range(heads):
                wqkv_v[l, pl.ds(pl.multiple_of(i * chunk_k, chunk_k), chunk_k), j * hh + h * hd:j * hh + (h + 1) * hd] = wtmp[pl.ds(h, chunk_k, stride=heads), :].astype(BF16)
            return carry
        lax.fori_loop(0, d_loc // chunk_k, body, 0)

    lane = lax.broadcasted_iota(jnp.int32, (rows, 128), 1)
    rown = lax.broadcasted_iota(jnp.int32, (rows, 128), 0)
    diag = lane == rown

    def norm_stage(n, p, gain):
        blocks = [xg[p, j].astype(F32) for j in range(nx)]
        sq = blocks[0] * blocks[0]
        for j in range(1, nx):
            sq = sq + blocks[j] * blocks[j]
        ssq = jnp.sum(sq, axis=1, keepdims=True)
        row = jnp.sum(jnp.where(diag, ssq, 0.0), axis=0, keepdims=True)
        ss_rx[n, my] = jnp.broadcast_to(row, (8, 128))
        inv = lax.rsqrt(ssq / d_loc + EPS)
        for j in range(nx):
            h_v[:, j * cb:(j + 1) * cb] = (blocks[j] * inv * gain[:, j * cb:(j + 1) * cb].astype(F32)).astype(BF16)

    def send_sums(n):
        for d in y_order:
            peer = lax.rem(my + d, ny)
            send(ss_rx.at[n, my], ss_rx.at[n, my], ss_ss.at[n, peer], ss_rs.at[n, my], {"y": peer})

    def ratio_rows(n):
        for d in y_order:
            src = lax.rem(my + d, ny)
            recv(ss_rx.at[n, src], ss_ss.at[n, src], ss_rs.at[n, src], {"y": src})
        parts = [ss_rx[n, s][0:1] for s in range(ny)]
        total = parts[0]
        for s in range(1, ny):
            total = total + parts[s]
        inv = lax.rsqrt(total / d_total + EPS)
        finite = total < jnp.inf
        return [jnp.where(finite, inv * jnp.sqrt(parts[s] / d_loc + EPS), 0.0) for s in range(ny)]

    def to_column(row, index):
        return jnp.sum(jnp.where(lax.broadcasted_iota(jnp.int32, index.shape, 1) == index, row, 0.0), axis=1, keepdims=True)

    def x_reduce(p, part, fill=None):
        for j in range(nx):
            rs_tx[p, j] = part[:, j * cb:(j + 1) * cb].astype(BF16)
        for d in x_order:
            dst = lax.rem(mx + d, nx)
            send(rs_tx.at[p, dst], rs_rx.at[p, mx], rs_ss.at[p, dst], rs_rs.at[p, mx], {"x": dst})
        if fill is not None:
            fill()
        total = xg[p, mx].astype(F32) + rs_tx[p, mx].astype(F32)
        for d in reversed(x_order):
            src = lax.rem(mx + d, nx)
            recv(rs_rx.at[p, src], rs_ss.at[p, src], rs_rs.at[p, src], {"x": src})
            total = total + rs_rx[p, src].astype(F32)
        xg[p + 1, mx] = total.astype(BF16)
        for d in x_order:
            dst = lax.rem(mx + d, nx)
            send(xg.at[p + 1, mx], xg.at[p + 1, mx], ag_ss.at[p, dst], ag_rs.at[p, mx], {"x": dst})

    def x_gather_wait(p):
        for d in range(1, nx):
            src = lax.rem(mx + d, nx)
            recv(xg.at[p + 1, src], ag_ss.at[p, src], ag_rs.at[p, src], {"x": src})

    loads["hid"].wait()
    for j in range(nx):
        xg[0, j] = hid_v[:, j * cb:(j + 1) * cb]
    key_lane = lax.broadcasted_iota(jnp.int32, (cells, kl), 1)
    key_row = lax.broadcasted_iota(jnp.int32, (cells, kl), 0)
    group_row = lax.broadcasted_iota(jnp.int32, (16, 1), 0) // heads
    per_group = 16 // heads

    def prepare_rel(l):
        pr = lax.broadcasted_iota(jnp.int32, (kl, kl), 0)
        pc = lax.broadcasted_iota(jnp.int32, (kl, kl), 1)
        flip = (pc == (seq - 1 - pr // heads) * heads + lax.rem(pr, heads)).astype(F32).astype(BF16)
        relf_v[l] = jnp.dot(flip, rel_v[l], preferred_element_type=F32).astype(BF16)
        first = rel_v[l, 0:16].astype(F32)
        for h in range(heads):
            r0_v[l, pl.ds(h, rb, stride=heads), :] = jnp.broadcast_to(first[h:h + 1], (rb, hd))

    def merge(l, new, tile_s, cache):
        for i in range(per_group):
            for h in range(heads):
                tile_s[pl.ds(i * heads + h, rb, stride=16), :] = new[:, h * hd:(h + 1) * hd]
        for b in range(rb):
            tile = tile_s[16 * b:16 * b + 16].astype(BF16)
            at = lent_s[16 * b:16 * b + 16].astype(BF16)
            full = jnp.broadcast_to(tile[None], (kl // 16, 16, hd)).reshape(kl, hd)
            where_at = jnp.broadcast_to(at[None], (kl // 16, 16, hd)).reshape(kl, hd)
            cache[l, b] = jnp.where(pos_v[...] == where_at, full, cache[l, b])

    def prepare_lengths():
        pos_v[...] = (lax.broadcasted_iota(jnp.int32, (kl, hd), 0) // heads).astype(F32).astype(BF16)
        index = my * rb + lax.broadcasted_iota(jnp.int32, (16 * rb, rows), 0) // 16
        lent_s[...] = jnp.broadcast_to(to_column(len_v[...].astype(F32), index), (16 * rb, hd))

    def early_relayout(l, j):
        loads["w", l, j].wait()
        relayout(l, j)

    fills = {}
    if layers > 1:
        fills = {"q": lambda l: early_relayout(l, 0), "up": lambda l: early_relayout(l, 1), "rs": lambda l: early_relayout(l, 2), "rs2": prepare_rel}

    def fill_for(name, l):
        return None if l >= layers or name not in fills else (lambda: fills[name](l))

    for l in range(layers):
        p = 2 * l
        if l == 0:
            loads["na"].wait()
        norm_stage(p, p, na_v[l:l + 1])
        if l:
            send_sums(p)
        for j in range(3):
            if l == 0:
                loads["w", 0, j].wait()
                relayout(0, j)
                if j == 0:
                    pl.semaphore_wait(barrier, ny - 1 + nx - 1)
                    send_sums(p)
            part = jnp.dot(h_v[...], wqkv_v[l, :, j * hh:(j + 1) * hh], preferred_element_type=F32)
            qkv_tx[l, j] = part.astype(BF16)
            for d in y_order:
                peer = lax.rem(my + d, ny)
                rows_at = pl.multiple_of(peer * rb, rb)
                send(qkv_tx.at[l, j, pl.ds(rows_at, rb)], qkv_rx.at[l, my, j], qkv_ss.at[l, j, peer], qkv_rs.at[l, j, my], {"y": peer})
        own_at = pl.multiple_of(my * rb, rb)
        for j in range(3):
            qkv_rx[l, my, j] = qkv_tx[l, j, pl.ds(own_at, rb), :]
        if l == 0:
            for name in ("len", "rel", "bu", "bw", "nm"):
                loads[name].wait()
            prepare_lengths()
            prepare_rel(0)
            if "q" in fills:
                fills["q"](1)
        loads["k", l].wait()
        loads["v", l].wait()
        lens_row = len_v[...].astype(F32)
        want = my * rb + lax.broadcasted_iota(jnp.int32, (cells, rows), 0) // heads
        lens = to_column(lens_row, want).astype(jnp.int32)
        ratios = ratio_rows(2 * l)
        want16 = my * rb + lax.broadcasted_iota(jnp.int32, (rb, 128), 0)
        cols = [to_column(r, want16) for r in ratios]

        def gathered(j):
            for d in y_order:
                src = lax.rem(my + d, ny)
                recv(qkv_rx.at[l, src, j], qkv_ss.at[l, j, src], qkv_rs.at[l, j, src], {"y": src})
            tot = qkv_rx[l, 0, j].astype(F32) * cols[0]
            for s in range(1, ny):
                tot = tot + qkv_rx[l, s, j].astype(F32) * cols[s]
            return tot.astype(BF16).astype(F32)

        q = gathered(0)
        for h in range(heads):
            qh = q[:, h * hd:(h + 1) * hd]
            a_s[pl.ds(h, rb, stride=heads), :] = qh + bu_v[l, h:h + 1].astype(F32)
            c_s[pl.ds(h, rb, stride=heads), :] = qh + bw_v[l, h:h + 1].astype(F32)
        a = a_s[...].astype(BF16)
        c = c_s[...].astype(BF16)
        rel = lax.dot_general(c, relf_v[l], (((1,), (1,)), ((), ())), preferred_element_type=F32)
        shift = seq - 1 - lens
        bit = 1
        while bit < seq:
            rolled = pltpu.roll(rel, kl - bit * heads, 1)
            rel = jnp.where(lax.rem(shift // bit, 2) == 1, rolled, rel)
            bit *= 2
        score_parts = []
        for g in range(cells // 16):
            ag = a[16 * g:16 * g + 16]
            sg = None
            for i in range(per_group):
                o = lax.dot_general(ag, kc_v[l, g * per_group + i], (((1,), (1,)), ((), ())), preferred_element_type=F32)
                sg = o if sg is None else jnp.where(group_row == i, o, sg)
            score_parts.append(sg)
        scores = jnp.concatenate(score_parts, axis=0)
        k = gathered(1)
        v = gathered(2)
        for h in range(heads):
            k_s[pl.ds(h, rb, stride=heads), :] = k[:, h * hd:(h + 1) * hd]
            v_s[pl.ds(h, rb, stride=heads), :] = v[:, h * hd:(h + 1) * hd]
        kn = k_s[...]
        vn = v_s[...]
        scale = hd ** -0.5
        s_new = (jnp.sum(a.astype(F32) * kn, axis=1, keepdims=True) + jnp.sum(c.astype(F32) * r0_v[l], axis=1, keepdims=True)) * scale
        valid = (lax.rem(key_lane, heads) == lax.rem(key_row, heads)) & (key_lane // heads < lens)
        scores = jnp.where(valid, (scores + rel) * scale, -jnp.inf)
        top = jnp.maximum(jnp.max(scores, axis=1, keepdims=True), s_new)
        e = jnp.exp(scores - top)
        e_new = jnp.exp(s_new - top)
        inv_den = 1.0 / (jnp.sum(e, axis=1, keepdims=True) + e_new)
        prob = (e * inv_den).astype(BF16)
        p_new = (e_new * inv_den).astype(BF16).astype(F32)
        ctx_parts = []
        for g in range(cells // 16):
            pg = prob[16 * g:16 * g + 16]
            cg = None
            for i in range(0, per_group, 2):
                b = g * per_group + i
                pair = jnp.concatenate([vc_v[l, b], vc_v[l, b + 1]], axis=1)
                o = jnp.dot(pg, pair, preferred_element_type=F32)
                cg = o[:, :hd] if cg is None else jnp.where(group_row == i, o[:, :hd], cg)
                cg = jnp.where(group_row == i + 1, o[:, hd:], cg)
            ctx_parts.append(cg)
        ctx_s[...] = jnp.concatenate(ctx_parts, axis=0) + p_new * vn
        for h in range(heads):
            ctx_all[l, my, :, h * hd:(h + 1) * hd] = ctx_s[pl.ds(h, rb, stride=heads), :].astype(BF16)
        for d in y_order:
            peer = lax.rem(my + d, ny)
            send(ctx_all.at[l, my], ctx_all.at[l, my], ctx_ss.at[l, peer], ctx_rs.at[l, my], {"y": peer})
        merge(l, k, kt_s, kc_v)
        merge(l, v, vt_s, vc_v)
        loads["o", l].wait()
        for d in reversed(y_order):
            src = lax.rem(my + d, ny)
            recv(ctx_all.at[l, src], ctx_ss.at[l, src], ctx_rs.at[l, src], {"y": src})
        ctx = jnp.concatenate([ctx_all[l, s] for s in range(ny)], axis=0)
        x_reduce(p, jnp.dot(ctx, wo_v[l], preferred_element_type=F32), fill_for("rs", l + 1))
        x_gather_wait(p)
        p = 2 * l + 1
        norm_stage(p, p, nm_v[l:l + 1])
        send_sums(p)
        loads["up", l].wait()
        for d in y_order + [0]:
            dst = lax.rem(my + d, ny)
            part = jnp.dot(h_v[...], wup_v[l, :, pl.ds(pl.multiple_of(dst * fb, fb), fb)], preferred_element_type=F32).astype(BF16)
            if d:
                up_tx[l, dst] = part
                send(up_tx.at[l, dst], up_rx.at[l, my], up_ss.at[l, dst], up_rs.at[l, my], {"y": dst})
            else:
                up_rx[l, my] = part
        if fill_for("up", l + 1) is not None:
            fills["up"](l + 1)
        ratios = ratio_rows(p)
        cols = [to_column(r, rown) for r in ratios]
        for d in y_order:
            src = lax.rem(my + d, ny)
            recv(up_rx.at[l, src], up_ss.at[l, src], up_rs.at[l, src], {"y": src})
        tot = up_rx[l, 0].astype(F32) * cols[0]
        for s in range(1, ny):
            tot = tot + up_rx[l, s].astype(F32) * cols[s]
        act[l, my] = jax.nn.gelu(tot.astype(BF16).astype(F32), approximate=True).astype(BF16)
        for d in y_order:
            peer = lax.rem(my + d, ny)
            send(act.at[l, my], act.at[l, my], act_ss.at[l, peer], act_rs.at[l, my], {"y": peer})
        loads["dn", l].wait()

        def down_rows(src):
            return pl.ds(pl.multiple_of(src * fb, fb), fb)

        acc_v[...] = jnp.dot(act[l, my], wdn_v[l, down_rows(my), :], preferred_element_type=F32)
        for d in reversed(y_order[1:]):
            src = lax.rem(my + d, ny)
            recv(act.at[l, src], act_ss.at[l, src], act_rs.at[l, src], {"y": src})
            acc_v[...] += jnp.dot(act[l, src], wdn_v[l, down_rows(src), :], preferred_element_type=F32)
        src = lax.rem(my + y_order[0], ny)
        recv(act.at[l, src], act_ss.at[l, src], act_rs.at[l, src], {"y": src})
        x_reduce(p, acc_v[...] + jnp.dot(act[l, src], wdn_v[l, down_rows(src), :], preferred_element_type=F32), fill_for("rs2", l + 1))
        x_gather_wait(p)

    last = 2 * layers
    for j in range(nx):
        hid_out[:, j * cb:(j + 1) * cb] = xg[last, j]
    for c in sends:
        c.wait_send()


def write_kernel(hid_in, kc_in, vc_in, hid_out, kc_out, vc_out, sem):
    copies = [pltpu.make_async_copy(hid_in, hid_out, sem.at[0])]
    layers, rb = kc_in.shape[:2]
    half = rb // 2
    for src, dst in ((kc_in, kc_out), (vc_in, vc_out)):
        for l in range(layers):
            for b in range(0, rb, half):
                copies.append(pltpu.make_async_copy(src.at[l, pl.ds(b, half)], dst.at[l, pl.ds(b, half)], sem.at[len(copies)]))
    for c in copies:
        c.start()
    for c in copies:
        c.wait()


def solution(mesh):
    ny = mesh.shape["y"]
    nx = mesh.shape["x"]
    cache_spec = P(None, ("rep", "y"), None, "x", None)
    row_spec = P("rep", "y")
    proj_spec = P(None, "y", "x", None)
    head_spec = P(None, "x", None)
    in_specs = (row_spec, P("rep"), cache_spec, cache_spec, P(None, None, "x", None), P(None, "y"),
                proj_spec, proj_spec, proj_spec, head_spec, head_spec, P(None, "x", None, "y"),
                P(None, "y"), P(None, "y", "x"), P(None, "x", "y"))
    out_specs = (row_spec, cache_spec, cache_spec)

    def local_step(hidden, lengths, k_cache, v_cache, rel_table, norm_attn, w_q, w_k, w_v, bias_content, bias_pos, w_out, norm_mlp, w_up, w_down):
        layers, rb, seq, heads, hd = k_cache.shape
        rows, d_loc = hidden.shape
        ff_loc = w_up.shape[2]
        hh = heads * hd
        cells = rb * heads
        kl = seq * heads
        cb = d_loc // nx
        fb = ff_loc // ny
        dims = (layers, ny, nx, rows, heads, hd, seq, d_loc, ff_loc)
        any_spec = pl.BlockSpec(memory_space=pl.ANY)
        vmem = pltpu.VMEM
        dma = pltpu.SemaphoreType.DMA
        scratch = [
            vmem((rows, d_loc), BF16), vmem((1, rows), jnp.int32),
            vmem((layers, kl, hd), BF16), vmem((layers, d_loc), BF16), vmem((layers, d_loc), BF16),
            vmem((layers, heads, hd), BF16), vmem((layers, heads, hd), BF16),
            vmem((layers, 3, d_loc * heads, hd), BF16), vmem((layers, d_loc, 3 * hh), BF16),
            vmem((layers, hh, d_loc), BF16), vmem((layers, d_loc, ff_loc), BF16), vmem((layers, ff_loc, d_loc), BF16),
            vmem((128 * heads, hd), F32), vmem((layers, kl, hd), BF16), vmem((layers, cells, hd), F32), vmem((rows, d_loc), BF16),
            vmem((cells, hd), F32), vmem((cells, hd), F32), vmem((cells, hd), F32), vmem((cells, hd), F32), vmem((cells, hd), F32),
            vmem((rows, d_loc), F32), vmem((kl, hd), BF16), vmem((16 * rb, hd), F32), vmem((16 * rb, hd), F32), vmem((16 * rb, hd), F32),
            vmem((2 * layers, ny, 8, 128), F32),
            vmem((layers, 3, rows, hh), BF16), vmem((layers, ny, 3, rb, hh), BF16), vmem((layers, ny, rb, hh), BF16),
            vmem((2 * layers, nx, rows, cb), BF16), vmem((2 * layers, nx, rows, cb), BF16), vmem((2 * layers + 1, nx, rows, cb), BF16),
            vmem((layers, ny, rows, fb), BF16), vmem((layers, ny, rows, fb), BF16), vmem((layers, ny, rows, fb), BF16),
            dma((7 + 8 * layers,)),
            dma((2 * layers, ny)), dma((2 * layers, ny)), dma((layers, 3, ny)), dma((layers, 3, ny)),
            dma((layers, ny)), dma((layers, ny)), dma((2 * layers, nx)), dma((2 * layers, nx)),
            dma((2 * layers, nx)), dma((2 * layers, nx)), dma((layers, ny)), dma((layers, ny)), dma((layers, ny)), dma((layers, ny)),
        ]
        cache_dims = (layers, rb, kl, hd)
        vmem_spec = pl.BlockSpec(memory_space=vmem)
        hid, k_new, v_new = pl.pallas_call(
            functools.partial(step_kernel, dims),
            out_shape=(vmem((rows, d_loc), BF16), vmem(cache_dims, BF16), vmem(cache_dims, BF16)),
            in_specs=[any_spec] * 15,
            out_specs=(vmem_spec,) * 3,
            scratch_shapes=scratch,
            compiler_params=pltpu.CompilerParams(collective_id=0, has_side_effects=True, vmem_limit_bytes=46 * 1024 * 1024),
            name="decode_step",
        )(hidden, lengths.reshape(1, rows), k_cache.reshape(layers, rb, kl, hd), v_cache.reshape(layers, rb, kl, hd),
          rel_table.reshape(layers, kl, hd), norm_attn,
          w_q.reshape(layers, d_loc * heads, hd), w_k.reshape(layers, d_loc * heads, hd), w_v.reshape(layers, d_loc * heads, hd),
          bias_content, bias_pos, w_out.reshape(layers, hh, d_loc), norm_mlp, w_up, w_down)

        flat = jax.ShapeDtypeStruct(cache_dims, BF16)
        hid, k_new, v_new = pl.pallas_call(
            write_kernel,
            out_shape=(jax.ShapeDtypeStruct((rows, d_loc), BF16), flat, flat),
            in_specs=[vmem_spec] * 3,
            out_specs=(any_spec,) * 3,
            scratch_shapes=[dma((1 + 4 * layers,))],
            compiler_params=pltpu.CompilerParams(vmem_limit_bytes=2 * 1024 * 1024),
            name="cache_write",
        )(hid, k_new, v_new)
        return hid, k_new.reshape(k_cache.shape), v_new.reshape(v_cache.shape)

    return jax.shard_map(local_step, mesh=mesh, in_specs=in_specs, out_specs=out_specs, check_vma=False)
```

```python
import functools

import jax
import jax.numpy as jnp
from jax import lax
from jax.experimental import pallas as pl
from jax.experimental.pallas import tpu as pltpu
from jax.sharding import PartitionSpec as P

EPS = 1e-6
F32 = jnp.float32
BF16 = jnp.bfloat16
MESH = pl.DeviceIdType.MESH


def step_kernel(dims, hidden_in, len_in, kc_in, vc_in, rel_in, na_in, wq_in, wk_in, wv_in, bu_in, bw_in, wo_in, nm_in, wup_in, wdn_in,
                hid_out, kc_v, vc_v,
                hid_v, len_v, rel_v, na_v, nm_v, bu_v, bw_v, wraw_v, wqkv_v, wo_v, wup_v, wdn_v,
                wtmp, relf_v, r0_v, h_v, a_s, c_s, k_s, v_s, ctx_s, acc_v, pos_v, lent_s, kt_s, vt_s, dg_v,
                ss_rx, qkv_tx, qkv_rx, ctx_all, rs_tx, rs_rx, xg, up_tx, up_rx, act,
                ld_sem, ss_ss, ss_rs, qkv_ss, qkv_rs, ctx_ss, ctx_rs, rs_ss, rs_rs, ag_ss, ag_rs, up_ss, up_rs, act_ss, act_rs):
    layers, ny, nx, rows, heads, hd, seq, d_loc, ff_loc = dims
    d_total = d_loc * ny
    rb = rows // ny
    hh = heads * hd
    cb = d_loc // nx
    fb = ff_loc // ny
    cells = rb * heads
    kl = seq * heads
    chips = nx // 2
    pair = 2 * cb
    fh = fb // 2
    my = lax.axis_index("y")
    mx = lax.axis_index("x")
    my_chip = mx // 2
    partner = mx + 1 - 2 * lax.rem(mx, 2)

    barrier = pltpu.get_barrier_semaphore()
    for d in range(1, ny):
        pl.semaphore_signal(barrier, inc=1, device_id={"y": lax.rem(my + d, ny)}, device_id_type=MESH)
    for d in range(1, nx):
        pl.semaphore_signal(barrier, inc=1, device_id={"x": lax.rem(mx + d, nx)}, device_id_type=MESH)

    loads = {}

    def load(name, src, dst):
        c = pltpu.make_async_copy(src, dst, ld_sem.at[len(loads)])
        c.start()
        loads[name] = c

    load("hid", hidden_in, hid_v)
    load("na", na_in, na_v)
    for j, w in enumerate((wq_in, wk_in, wv_in)):
        load(("w", 0, j), w.at[0], wraw_v.at[0, j])
    load("len", len_in, len_v)
    load("rel", rel_in, rel_v)
    load("bu", bu_in, bu_v)
    load("bw", bw_in, bw_v)
    load("nm", nm_in, nm_v)
    load(("k", 0), kc_in.at[0], kc_v.at[0])
    load(("v", 0), vc_in.at[0], vc_v.at[0])
    load(("o", 0), wo_in.at[0], wo_v.at[0])
    load(("up", 0), wup_in.at[0], wup_v.at[0])
    load(("dn", 0), wdn_in.at[0], wdn_v.at[0])
    for l in range(1, layers):
        for j, w in enumerate((wq_in, wk_in, wv_in)):
            load(("w", l, j), w.at[l], wraw_v.at[l, j])
        load(("k", l), kc_in.at[l], kc_v.at[l])
        load(("v", l), vc_in.at[l], vc_v.at[l])
        load(("o", l), wo_in.at[l], wo_v.at[l])
        load(("up", l), wup_in.at[l], wup_v.at[l])
        load(("dn", l), wdn_in.at[l], wdn_v.at[l])

    sends = []

    def send(src, dst, ss, rs, dev):
        c = pltpu.make_async_remote_copy(src_ref=src, dst_ref=dst, send_sem=ss, recv_sem=rs, device_id=dev, device_id_type=MESH)
        c.start()
        sends.append(c)

    def recv(dst, ss, rs, dev):
        pltpu.make_async_remote_copy(src_ref=dst, dst_ref=dst, send_sem=ss, recv_sem=rs, device_id=dev, device_id_type=MESH).wait_recv()

    x_order = sorted(range(1, nx), key=lambda d: -min(d, nx - d))
    y_order = [2, 1, 3] if ny == 4 else list(range(1, ny))
    chunk_k = 128
    chunk = chunk_k * heads

    def relayout(l, j):
        def body(i, carry):
            wtmp[...] = wraw_v[l, j, pl.ds(pl.multiple_of(i * chunk, chunk), chunk), :].astype(F32)
            for h in range(heads):
                wqkv_v[l, pl.ds(pl.multiple_of(i * chunk_k, chunk_k), chunk_k), j * hh + h * hd:j * hh + (h + 1) * hd] = wtmp[pl.ds(h, chunk_k, stride=heads), :].astype(BF16)
            return carry
        lax.fori_loop(0, d_loc // chunk_k, body, 0)

    lane = lax.broadcasted_iota(jnp.int32, (rows, 128), 1)
    rown = lax.broadcasted_iota(jnp.int32, (rows, 128), 0)
    diag = lane == rown

    def store_sums(n, ssq):
        row = jnp.sum(jnp.where(diag, ssq, 0.0), axis=0, keepdims=True)
        ss_rx[n, my] = jnp.broadcast_to(row, (8, 128))

    def norm_stage(n, p, gain):
        blocks = [xg[p, j].astype(F32) for j in range(nx)]
        sq = blocks[0] * blocks[0]
        for j in range(1, nx):
            sq = sq + blocks[j] * blocks[j]
        ssq = jnp.sum(sq, axis=1, keepdims=True)
        store_sums(n, ssq)
        inv = lax.rsqrt(ssq / d_loc + EPS)
        for j in range(nx):
            h_v[:, j * cb:(j + 1) * cb] = (blocks[j] * inv * gain[:, j * cb:(j + 1) * cb].astype(F32)).astype(BF16)

    def send_sums(n):
        for d in y_order:
            peer = lax.rem(my + d, ny)
            send(ss_rx.at[n, my], ss_rx.at[n, my], ss_ss.at[n, peer], ss_rs.at[n, my], {"y": peer})

    def ratio_rows(n):
        for d in y_order:
            src = lax.rem(my + d, ny)
            recv(ss_rx.at[n, src], ss_ss.at[n, src], ss_rs.at[n, src], {"y": src})
        parts = [ss_rx[n, s][0:1] for s in range(ny)]
        total = parts[0]
        for s in range(1, ny):
            total = total + parts[s]
        inv = lax.rsqrt(total / d_total + EPS)
        finite = total < jnp.inf
        return [jnp.where(finite, inv * jnp.sqrt(parts[s] / d_loc + EPS), 0.0) for s in range(ny)]

    def to_column(row, index):
        return jnp.sum(jnp.where(lax.broadcasted_iota(jnp.int32, index.shape, 1) == index, row, 0.0), axis=1, keepdims=True)

    def x_reduce(p, part, fill=None):
        for j in range(nx):
            rs_tx[p, j] = part[:, j * cb:(j + 1) * cb].astype(BF16)
        for d in x_order:
            dst = lax.rem(mx + d, nx)
            send(rs_tx.at[p, dst], rs_rx.at[p, mx], rs_ss.at[p, dst], rs_rs.at[p, mx], {"x": dst})
        if fill is not None:
            fill()
        total = xg[p, mx].astype(F32) + rs_tx[p, mx].astype(F32)
        for d in reversed(x_order):
            src = lax.rem(mx + d, nx)
            recv(rs_rx.at[p, src], rs_ss.at[p, src], rs_rs.at[p, src], {"x": src})
            total = total + rs_rx[p, src].astype(F32)
        xg[p + 1, mx] = total.astype(BF16)
        for d in x_order:
            dst = lax.rem(mx + d, nx)
            send(xg.at[p + 1, mx], xg.at[p + 1, mx], ag_ss.at[p, dst], ag_rs.at[p, mx], {"x": dst})

    def recv_block(p, src):
        recv(xg.at[p + 1, src], ag_ss.at[p, src], ag_rs.at[p, src], {"x": src})

    groups = [[0]] + [sorted({d, chips - d}) for d in range(1, chips // 2 + 1)]

    def scaled(p, gain, l, group):
        at = [lax.rem(my_chip + dc, chips) for dc in group]
        for dc, chip in zip(group, at):
            if dc == 0:
                recv_block(p, partner)
            else:
                recv_block(p, 2 * chip)
                recv_block(p, 2 * chip + 1)
        blocks = [jnp.concatenate([xg[p + 1, 2 * chip], xg[p + 1, 2 * chip + 1]], axis=1).astype(F32) for chip in at]
        ssq = jnp.sum(sum(b * b for b in blocks), axis=1, keepdims=True)
        inv = lax.rsqrt(ssq / (pair * len(group)) + EPS)
        spans = [pl.ds(pl.multiple_of(chip * pair, pair), pair) for chip in at]
        return ssq, [((b * inv * gain[l:l + 1, sp].astype(F32)).astype(BF16), sp) for b, sp in zip(blocks, spans)]

    def gather_matmul(n, p, gain, l, weight, columns):
        sums = []
        for i, group in enumerate(groups):
            ssq, hs = scaled(p, gain, l, group)
            sums.append(ssq)
            if i + 1 < len(groups):
                for c in range(0, columns, 512):
                    dg_v[i, :, c:c + 512] = sum(jnp.dot(h, weight[l, sp, c:c + 512], preferred_element_type=F32) for h, sp in hs)
        total = sum(sums)
        store_sums(n, total)
        send_sums(n)
        inv = lax.rsqrt(total / d_loc + EPS)
        factors = [jnp.where(total < jnp.inf, inv * jnp.sqrt(q / (pair * len(g)) + EPS), 0.0) for q, g in zip(sums, groups)]

        def product(c, width):
            last = sum(jnp.dot(h, weight[l, sp, c:c + width], preferred_element_type=F32) for h, sp in hs)
            return sum(f * dg_v[i, :, c:c + width] for i, f in enumerate(factors[:-1])) + factors[-1] * last
        return product

    loads["hid"].wait()
    for j in range(nx):
        xg[0, j] = hid_v[:, j * cb:(j + 1) * cb]
    key_lane = lax.broadcasted_iota(jnp.int32, (cells, kl), 1)
    key_row = lax.broadcasted_iota(jnp.int32, (cells, kl), 0)
    group_row = lax.broadcasted_iota(jnp.int32, (16, 1), 0) // heads
    per_group = 16 // heads

    def prepare_rel(l):
        pr = lax.broadcasted_iota(jnp.int32, (kl, kl), 0)
        pc = lax.broadcasted_iota(jnp.int32, (kl, kl), 1)
        flip = (pc == (seq - 1 - pr // heads) * heads + lax.rem(pr, heads)).astype(F32).astype(BF16)
        relf_v[l] = jnp.dot(flip, rel_v[l], preferred_element_type=F32).astype(BF16)
        first = rel_v[l, 0:16].astype(F32)
        for h in range(heads):
            r0_v[l, pl.ds(h, rb, stride=heads), :] = jnp.broadcast_to(first[h:h + 1], (rb, hd))

    def merge(l, new, tile_s, cache):
        for i in range(per_group):
            for h in range(heads):
                tile_s[pl.ds(i * heads + h, rb, stride=16), :] = new[:, h * hd:(h + 1) * hd]
        for b in range(rb):
            tile = tile_s[16 * b:16 * b + 16].astype(BF16)
            at = lent_s[16 * b:16 * b + 16].astype(BF16)
            full = jnp.broadcast_to(tile[None], (kl // 16, 16, hd)).reshape(kl, hd)
            where_at = jnp.broadcast_to(at[None], (kl // 16, 16, hd)).reshape(kl, hd)
            cache[l, b] = jnp.where(pos_v[...] == where_at, full, cache[l, b])

    def prepare_lengths():
        pos_v[...] = (lax.broadcasted_iota(jnp.int32, (kl, hd), 0) // heads).astype(F32).astype(BF16)
        index = my * rb + lax.broadcasted_iota(jnp.int32, (16 * rb, rows), 0) // 16
        lent_s[...] = jnp.broadcast_to(to_column(len_v[...].astype(F32), index), (16 * rb, hd))

    def early_relayout(l, j):
        loads["w", l, j].wait()
        relayout(l, j)

    fills = {}
    if layers > 1:
        fills = {"q": lambda l: early_relayout(l, 0), "up": lambda l: early_relayout(l, 1), "rs": lambda l: early_relayout(l, 2), "rs2": prepare_rel}

    def fill_for(name, l):
        return None if l >= layers or name not in fills else (lambda: fills[name](l))

    for l in range(layers):
        p = 2 * l
        def send_qkv(j):
            for d in y_order:
                peer = lax.rem(my + d, ny)
                rows_at = pl.multiple_of(peer * rb, rb)
                send(qkv_tx.at[l, j, pl.ds(rows_at, rb)], qkv_rx.at[l, my, j], qkv_ss.at[l, j, peer], qkv_rs.at[l, j, my], {"y": peer})

        if l == 0:
            loads["na"].wait()
            norm_stage(p, p, na_v[l:l + 1])
            for j in range(3):
                early_relayout(0, j)
                qkv_tx[l, j] = jnp.dot(h_v[...], wqkv_v[l, :, j * hh:(j + 1) * hh], preferred_element_type=F32).astype(BF16)
                if j == 1:
                    pl.semaphore_wait(barrier, ny - 1 + nx - 1)
                    send_sums(p)
                    send_qkv(0)
                if j:
                    send_qkv(j)
        else:
            product = gather_matmul(p, p - 1, na_v, l, wqkv_v, 3 * hh)
            for j in range(3):
                qkv_tx[l, j] = product(j * hh, hh).astype(BF16)
                send_qkv(j)
        own_at = pl.multiple_of(my * rb, rb)
        for j in range(3):
            qkv_rx[l, my, j] = qkv_tx[l, j, pl.ds(own_at, rb), :]
        if l == 0:
            for name in ("len", "rel", "bu", "bw", "nm"):
                loads[name].wait()
            prepare_rel(0)
        loads["k", l].wait()
        loads["v", l].wait()
        lens_row = len_v[...].astype(F32)
        want = my * rb + lax.broadcasted_iota(jnp.int32, (cells, rows), 0) // heads
        lens = to_column(lens_row, want).astype(jnp.int32)
        ratios = ratio_rows(2 * l)
        want16 = my * rb + lax.broadcasted_iota(jnp.int32, (rb, 128), 0)
        cols = [to_column(r, want16) for r in ratios]

        def gathered(j):
            for d in y_order:
                src = lax.rem(my + d, ny)
                recv(qkv_rx.at[l, src, j], qkv_ss.at[l, j, src], qkv_rs.at[l, j, src], {"y": src})
            tot = qkv_rx[l, 0, j].astype(F32) * cols[0]
            for s in range(1, ny):
                tot = tot + qkv_rx[l, s, j].astype(F32) * cols[s]
            return tot.astype(BF16).astype(F32)

        q = gathered(0)
        for h in range(heads):
            qh = q[:, h * hd:(h + 1) * hd]
            a_s[pl.ds(h, rb, stride=heads), :] = qh + bu_v[l, h:h + 1].astype(F32)
            c_s[pl.ds(h, rb, stride=heads), :] = qh + bw_v[l, h:h + 1].astype(F32)
        a = a_s[...].astype(BF16)
        c = c_s[...].astype(BF16)
        rel = lax.dot_general(c, relf_v[l], (((1,), (1,)), ((), ())), preferred_element_type=F32)
        shift = seq - 1 - lens
        bit = 1
        while bit < seq:
            rolled = pltpu.roll(rel, kl - bit * heads, 1)
            rel = jnp.where(lax.rem(shift // bit, 2) == 1, rolled, rel)
            bit *= 2
        score_parts = []
        for g in range(cells // 16):
            ag = a[16 * g:16 * g + 16]
            sg = None
            for i in range(per_group):
                o = lax.dot_general(ag, kc_v[l, g * per_group + i], (((1,), (1,)), ((), ())), preferred_element_type=F32)
                sg = o if sg is None else jnp.where(group_row == i, o, sg)
            score_parts.append(sg)
        scores = jnp.concatenate(score_parts, axis=0)
        k = gathered(1)
        v = gathered(2)
        for h in range(heads):
            k_s[pl.ds(h, rb, stride=heads), :] = k[:, h * hd:(h + 1) * hd]
            v_s[pl.ds(h, rb, stride=heads), :] = v[:, h * hd:(h + 1) * hd]
        kn = k_s[...]
        vn = v_s[...]
        scale = hd ** -0.5
        s_new = (jnp.sum(a.astype(F32) * kn, axis=1, keepdims=True) + jnp.sum(c.astype(F32) * r0_v[l], axis=1, keepdims=True)) * scale
        valid = (lax.rem(key_lane, heads) == lax.rem(key_row, heads)) & (key_lane // heads < lens)
        scores = jnp.where(valid, (scores + rel) * scale, -jnp.inf)
        top = jnp.maximum(jnp.max(scores, axis=1, keepdims=True), s_new)
        e = jnp.exp(scores - top)
        e_new = jnp.exp(s_new - top)
        inv_den = 1.0 / (jnp.sum(e, axis=1, keepdims=True) + e_new)
        prob = (e * inv_den).astype(BF16)
        p_new = (e_new * inv_den).astype(BF16).astype(F32)
        ctx_parts = []
        for g in range(cells // 16):
            pg = prob[16 * g:16 * g + 16]
            cg = None
            for i in range(0, per_group, 2):
                b = g * per_group + i
                values = jnp.concatenate([vc_v[l, b], vc_v[l, b + 1]], axis=1)
                o = jnp.dot(pg, values, preferred_element_type=F32)
                cg = o[:, :hd] if cg is None else jnp.where(group_row == i, o[:, :hd], cg)
                cg = jnp.where(group_row == i + 1, o[:, hd:], cg)
            ctx_parts.append(cg)
        ctx_s[...] = jnp.concatenate(ctx_parts, axis=0) + p_new * vn
        for h in range(heads):
            ctx_all[l, my, :, h * hd:(h + 1) * hd] = ctx_s[pl.ds(h, rb, stride=heads), :].astype(BF16)
        for d in y_order:
            peer = lax.rem(my + d, ny)
            send(ctx_all.at[l, my], ctx_all.at[l, my], ctx_ss.at[l, peer], ctx_rs.at[l, my], {"y": peer})
        if l == 0:
            prepare_lengths()
        if fill_for("q", l + 1) is not None:
            fills["q"](l + 1)
        merge(l, k, kt_s, kc_v)
        merge(l, v, vt_s, vc_v)
        loads["o", l].wait()
        for d in reversed(y_order):
            src = lax.rem(my + d, ny)
            recv(ctx_all.at[l, src], ctx_ss.at[l, src], ctx_rs.at[l, src], {"y": src})
        ctx = jnp.concatenate([ctx_all[l, s] for s in range(ny)], axis=0)
        x_reduce(p, jnp.dot(ctx, wo_v[l], preferred_element_type=F32), fill_for("rs", l + 1))
        p = 2 * l + 1
        loads["up", l].wait()
        product = gather_matmul(p, p - 1, nm_v, l, wup_v, ff_loc)
        for hf in range(2):
            for j in range(ny):
                up_tx[l, hf, j] = product(j * fb + hf * fh, fh).astype(BF16)
            for d in y_order:
                dst = lax.rem(my + d, ny)
                send(up_tx.at[l, hf, dst], up_rx.at[l, hf, my], up_ss.at[l, hf, dst], up_rs.at[l, hf, my], {"y": dst})
        for hf in range(2):
            up_rx[l, hf, my] = up_tx[l, hf, my]
        if fill_for("up", l + 1) is not None:
            fills["up"](l + 1)
        ratios = ratio_rows(p)
        cols = [to_column(r, rown) for r in ratios]
        loads["dn", l].wait()
        for hf in range(2):
            for d in reversed(y_order):
                src = lax.rem(my + d, ny)
                recv(up_rx.at[l, hf, src], up_ss.at[l, hf, src], up_rs.at[l, hf, src], {"y": src})
            tot = up_rx[l, hf, 0].astype(F32) * cols[0]
            for s in range(1, ny):
                tot = tot + up_rx[l, hf, s].astype(F32) * cols[s]
            act[l, hf, my] = jax.nn.gelu(tot.astype(BF16).astype(F32), approximate=True).astype(BF16)
            for d in y_order:
                peer = lax.rem(my + d, ny)
                send(act.at[l, hf, my], act.at[l, hf, my], act_ss.at[l, hf, peer], act_rs.at[l, hf, my], {"y": peer})

        def down(hf, src):
            return jnp.dot(act[l, hf, src], wdn_v[l, pl.ds(pl.multiple_of(src * fb + hf * fh, fh), fh), :], preferred_element_type=F32)

        acc_v[...] = down(0, my) + down(1, my)
        pieces = [(hf, d) for hf in range(2) for d in reversed(y_order)]
        for hf, d in pieces:
            src = lax.rem(my + d, ny)
            recv(act.at[l, hf, src], act_ss.at[l, hf, src], act_rs.at[l, hf, src], {"y": src})
            if (hf, d) != pieces[-1]:
                acc_v[...] += down(hf, src)
        x_reduce(p, acc_v[...] + down(hf, src), fill_for("rs2", l + 1))
    for d in range(1, nx):
        recv_block(2 * layers - 1, lax.rem(mx + d, nx))

    last = 2 * layers
    for j in range(nx):
        hid_out[:, j * cb:(j + 1) * cb] = xg[last, j]
    for c in sends:
        c.wait_send()


def write_kernel(hid_in, kc_in, vc_in, hid_out, kc_out, vc_out, sem):
    copies = [pltpu.make_async_copy(hid_in, hid_out, sem.at[0])]
    layers, rb = kc_in.shape[:2]
    half = rb // 2
    for src, dst in ((kc_in, kc_out), (vc_in, vc_out)):
        for l in range(layers):
            for b in range(0, rb, half):
                copies.append(pltpu.make_async_copy(src.at[l, pl.ds(b, half)], dst.at[l, pl.ds(b, half)], sem.at[len(copies)]))
    for c in copies:
        c.start()
    for c in copies:
        c.wait()


def solution(mesh):
    ny = mesh.shape["y"]
    nx = mesh.shape["x"]
    cache_spec = P(None, ("rep", "y"), None, "x", None)
    row_spec = P("rep", "y")
    proj_spec = P(None, "y", "x", None)
    head_spec = P(None, "x", None)
    in_specs = (row_spec, P("rep"), cache_spec, cache_spec, P(None, None, "x", None), P(None, "y"),
                proj_spec, proj_spec, proj_spec, head_spec, head_spec, P(None, "x", None, "y"),
                P(None, "y"), P(None, "y", "x"), P(None, "x", "y"))
    out_specs = (row_spec, cache_spec, cache_spec)

    def local_step(hidden, lengths, k_cache, v_cache, rel_table, norm_attn, w_q, w_k, w_v, bias_content, bias_pos, w_out, norm_mlp, w_up, w_down):
        layers, rb, seq, heads, hd = k_cache.shape
        rows, d_loc = hidden.shape
        ff_loc = w_up.shape[2]
        hh = heads * hd
        cells = rb * heads
        kl = seq * heads
        cb = d_loc // nx
        fb = ff_loc // ny
        dims = (layers, ny, nx, rows, heads, hd, seq, d_loc, ff_loc)
        any_spec = pl.BlockSpec(memory_space=pl.ANY)
        vmem = pltpu.VMEM
        dma = pltpu.SemaphoreType.DMA
        scratch = [
            vmem((rows, d_loc), BF16), vmem((1, rows), jnp.int32),
            vmem((layers, kl, hd), BF16), vmem((layers, d_loc), BF16), vmem((layers, d_loc), BF16),
            vmem((layers, heads, hd), BF16), vmem((layers, heads, hd), BF16),
            vmem((layers, 3, d_loc * heads, hd), BF16), vmem((layers, d_loc, 3 * hh), BF16),
            vmem((layers, hh, d_loc), BF16), vmem((layers, d_loc, ff_loc), BF16), vmem((layers, ff_loc, d_loc), BF16),
            vmem((128 * heads, hd), F32), vmem((layers, kl, hd), BF16), vmem((layers, cells, hd), F32), vmem((rows, d_loc), BF16),
            vmem((cells, hd), F32), vmem((cells, hd), F32), vmem((cells, hd), F32), vmem((cells, hd), F32), vmem((cells, hd), F32),
            vmem((rows, d_loc), F32), vmem((kl, hd), BF16), vmem((16 * rb, hd), F32), vmem((16 * rb, hd), F32), vmem((16 * rb, hd), F32),
            vmem((nx // 4, rows, max(ff_loc, 3 * hh)), F32),
            vmem((2 * layers, ny, 8, 128), F32),
            vmem((layers, 3, rows, hh), BF16), vmem((layers, ny, 3, rb, hh), BF16), vmem((layers, ny, rb, hh), BF16),
            vmem((2 * layers, nx, rows, cb), BF16), vmem((2 * layers, nx, rows, cb), BF16), vmem((2 * layers + 1, nx, rows, cb), BF16),
            vmem((layers, 2, ny, rows, fb // 2), BF16), vmem((layers, 2, ny, rows, fb // 2), BF16), vmem((layers, 2, ny, rows, fb // 2), BF16),
            dma((7 + 8 * layers,)),
            dma((2 * layers, ny)), dma((2 * layers, ny)), dma((layers, 3, ny)), dma((layers, 3, ny)),
            dma((layers, ny)), dma((layers, ny)), dma((2 * layers, nx)), dma((2 * layers, nx)),
            dma((2 * layers, nx)), dma((2 * layers, nx)), dma((layers, 2, ny)), dma((layers, 2, ny)), dma((layers, 2, ny)), dma((layers, 2, ny)),
        ]
        cache_dims = (layers, rb, kl, hd)
        vmem_spec = pl.BlockSpec(memory_space=vmem)
        hid, k_new, v_new = pl.pallas_call(
            functools.partial(step_kernel, dims),
            out_shape=(vmem((rows, d_loc), BF16), vmem(cache_dims, BF16), vmem(cache_dims, BF16)),
            in_specs=[any_spec] * 15,
            out_specs=(vmem_spec,) * 3,
            scratch_shapes=scratch,
            compiler_params=pltpu.CompilerParams(collective_id=0, has_side_effects=True, vmem_limit_bytes=46 * 1024 * 1024),
            name="decode_step",
        )(hidden, lengths.reshape(1, rows), k_cache.reshape(layers, rb, kl, hd), v_cache.reshape(layers, rb, kl, hd),
          rel_table.reshape(layers, kl, hd), norm_attn,
          w_q.reshape(layers, d_loc * heads, hd), w_k.reshape(layers, d_loc * heads, hd), w_v.reshape(layers, d_loc * heads, hd),
          bias_content, bias_pos, w_out.reshape(layers, hh, d_loc), norm_mlp, w_up, w_down)

        flat = jax.ShapeDtypeStruct(cache_dims, BF16)
        hid, k_new, v_new = pl.pallas_call(
            write_kernel,
            out_shape=(jax.ShapeDtypeStruct((rows, d_loc), BF16), flat, flat),
            in_specs=[vmem_spec] * 3,
            out_specs=(any_spec,) * 3,
            scratch_shapes=[dma((1 + 4 * layers,))],
            compiler_params=pltpu.CompilerParams(vmem_limit_bytes=2 * 1024 * 1024),
            name="cache_write",
        )(hid, k_new, v_new)
        return hid, k_new.reshape(k_cache.shape), v_new.reshape(v_cache.shape)

    return jax.shard_map(local_step, mesh=mesh, in_specs=in_specs, out_specs=out_specs, check_vma=False)
```

```python
import functools

import jax
import jax.numpy as jnp
from jax import lax
from jax.experimental import pallas as pl
from jax.experimental.pallas import tpu as pltpu
from jax.sharding import PartitionSpec as P

EPS = 1e-6
F32 = jnp.float32
BF16 = jnp.bfloat16
MESH = pl.DeviceIdType.MESH


def step_kernel(dims, hidden_in, len_in, kc_in, vc_in, rel_in, na_in, wq_in, wk_in, wv_in, bu_in, bw_in, wo_in, nm_in, wup_in, wdn_in,
                hid_out, kc_v, vc_v,
                hid_v, len_v, rel_v, na_v, nm_v, bu_v, bw_v, wraw_v, wqkv_v, wo_v, wup_v, wdn_v,
                wtmp, relf_v, r0_v, h_v, a_s, c_s, k_s, v_s, ctx_s, acc_v, pos_v, lent_s, kt_s, vt_s, dg_v,
                ss_rx, qkv_tx, qkv_rx, ctx_all, dd_tx, dd_rx, bc, xh, up_tx, up_rx, act,
                ld_sem, ss_ss, ss_rs, qkv_ss, qkv_rs, ctx_ss, ctx_rs, dd_ss, dd_rs, bc_ss, bc_rs, xe_ss, xe_rs, up_ss, up_rs, act_ss, act_rs):
    layers, ny, nx, rows, heads, hd, seq, d_loc, ff_loc = dims
    d_total = d_loc * ny
    rb = rows // ny
    hh = heads * hd
    half = d_loc // 2
    fb = ff_loc // ny
    cells = rb * heads
    kl = seq * heads
    chips = nx // 2
    fh = fb // 2
    my = lax.axis_index("y")
    mx = lax.axis_index("x")
    my_chip = mx // 2
    core = lax.rem(mx, 2)
    other = 1 - core
    partner = {"x": 2 * my_chip + other}

    barrier = pltpu.get_barrier_semaphore()
    for d in range(1, ny):
        pl.semaphore_signal(barrier, inc=1, device_id={"y": lax.rem(my + d, ny)}, device_id_type=MESH)
    pl.semaphore_signal(barrier, inc=1, device_id=partner, device_id_type=MESH)
    for d in range(1, chips):
        pl.semaphore_signal(barrier, inc=1, device_id={"x": 2 * lax.rem(my_chip + d, chips) + core}, device_id_type=MESH)

    loads = {}

    def load(name, src, dst):
        c = pltpu.make_async_copy(src, dst, ld_sem.at[len(loads)])
        c.start()
        loads[name] = c

    load("hid", hidden_in, hid_v)
    load("na", na_in, na_v)
    for j, w in enumerate((wq_in, wk_in, wv_in)):
        load(("w", 0, j), w.at[0], wraw_v.at[0, j])
    load("len", len_in, len_v)
    load("rel", rel_in, rel_v)
    load("bu", bu_in, bu_v)
    load("bw", bw_in, bw_v)
    load("nm", nm_in, nm_v)
    load(("k", 0), kc_in.at[0], kc_v.at[0])
    load(("v", 0), vc_in.at[0], vc_v.at[0])
    load(("o", 0), wo_in.at[0], wo_v.at[0])
    load(("up", 0), wup_in.at[0], wup_v.at[0])
    load(("dn", 0), wdn_in.at[0], wdn_v.at[0])
    for l in range(1, layers):
        for j, w in enumerate((wq_in, wk_in, wv_in)):
            load(("w", l, j), w.at[l], wraw_v.at[l, j])
        load(("k", l), kc_in.at[l], kc_v.at[l])
        load(("v", l), vc_in.at[l], vc_v.at[l])
        load(("o", l), wo_in.at[l], wo_v.at[l])
        load(("up", l), wup_in.at[l], wup_v.at[l])
        load(("dn", l), wdn_in.at[l], wdn_v.at[l])

    sends = []

    def send(src, dst, ss, rs, dev):
        c = pltpu.make_async_remote_copy(src_ref=src, dst_ref=dst, send_sem=ss, recv_sem=rs, device_id=dev, device_id_type=MESH)
        c.start()
        sends.append(c)

    def recv(dst, ss, rs, dev):
        pltpu.make_async_remote_copy(src_ref=dst, dst_ref=dst, send_sem=ss, recv_sem=rs, device_id=dev, device_id_type=MESH).wait_recv()

    chip_order = sorted(range(1, chips), key=lambda d: -min(d, chips - d))
    y_order = [2, 1, 3] if ny == 4 else list(range(1, ny))
    chunk_k = 128
    chunk = chunk_k * heads

    def relayout(l, j):
        def body(i, carry):
            wtmp[...] = wraw_v[l, j, pl.ds(pl.multiple_of(i * chunk, chunk), chunk), :].astype(F32)
            for h in range(heads):
                wqkv_v[l, pl.ds(pl.multiple_of(i * chunk_k, chunk_k), chunk_k), j * hh + h * hd:j * hh + (h + 1) * hd] = wtmp[pl.ds(h, chunk_k, stride=heads), :].astype(BF16)
            return carry
        lax.fori_loop(0, d_loc // chunk_k, body, 0)

    lane = lax.broadcasted_iota(jnp.int32, (rows, 128), 1)
    rown = lax.broadcasted_iota(jnp.int32, (rows, 128), 0)
    diag = lane == rown

    def store_sums(n, ssq):
        row = jnp.sum(jnp.where(diag, ssq, 0.0), axis=0, keepdims=True)
        ss_rx[n, my] = jnp.broadcast_to(row, (8, 128))

    def norm_stage(n, p, gain):
        blocks = [xh[p, j].astype(F32) for j in range(2)]
        ssq = jnp.sum(sum(b * b for b in blocks), axis=1, keepdims=True)
        store_sums(n, ssq)
        inv = lax.rsqrt(ssq / d_loc + EPS)
        for j in range(2):
            h_v[:, j * half:(j + 1) * half] = (blocks[j] * inv * gain[:, j * half:(j + 1) * half].astype(F32)).astype(BF16)

    def send_sums(n):
        for d in y_order:
            peer = lax.rem(my + d, ny)
            send(ss_rx.at[n, my], ss_rx.at[n, my], ss_ss.at[n, peer], ss_rs.at[n, my], {"y": peer})

    def ratio_rows(n):
        for d in y_order:
            src = lax.rem(my + d, ny)
            recv(ss_rx.at[n, src], ss_ss.at[n, src], ss_rs.at[n, src], {"y": src})
        parts = [ss_rx[n, s][0:1] for s in range(ny)]
        total = parts[0]
        for s in range(1, ny):
            total = total + parts[s]
        inv = lax.rsqrt(total / d_total + EPS)
        finite = total < jnp.inf
        return [jnp.where(finite, inv * jnp.sqrt(parts[s] / d_loc + EPS), 0.0) for s in range(ny)]

    def to_column(row, index):
        return jnp.sum(jnp.where(lax.broadcasted_iota(jnp.int32, index.shape, 1) == index, row, 0.0), axis=1, keepdims=True)

    def half_at(which):
        return pl.ds(pl.multiple_of(which * half, half), half)

    def x_reduce(p, part, fill=None):
        dd_tx[p] = part(half_at(other)).astype(BF16)
        send(dd_tx.at[p], dd_rx.at[p], dd_ss.at[p], dd_rs.at[p], partner)
        own = part(half_at(core))
        recv(dd_rx.at[p], dd_ss.at[p], dd_rs.at[p], partner)
        bc[p, my_chip] = (own + dd_rx[p].astype(F32)).astype(BF16)
        for d in chip_order:
            chip = lax.rem(my_chip + d, chips)
            send(bc.at[p, my_chip], bc.at[p, my_chip], bc_ss.at[p, chip], bc_rs.at[p, my_chip], {"x": 2 * chip + core})
        if fill is not None:
            fill()
        for d in reversed(chip_order):
            chip = lax.rem(my_chip + d, chips)
            recv(bc.at[p, chip], bc_ss.at[p, chip], bc_rs.at[p, chip], {"x": 2 * chip + core})
        total = xh[p, core].astype(F32)
        for chip in range(chips):
            total = total + bc[p, chip].astype(F32)
        xh[p + 1, core] = total.astype(BF16)
        send(xh.at[p + 1, core], xh.at[p + 1, core], xe_ss.at[p], xe_rs.at[p], partner)

    def recv_half(p):
        recv(xh.at[p + 1, other], xe_ss.at[p], xe_rs.at[p], partner)

    groups = [core, other]

    def scaled(p, gain, l, which):
        block = xh[p + 1, which].astype(F32)
        ssq = jnp.sum(block * block, axis=1, keepdims=True)
        inv = lax.rsqrt(ssq / half + EPS)
        at = half_at(which)
        return ssq, [((block * inv * gain[l:l + 1, at].astype(F32)).astype(BF16), at)]

    def gather_matmul(n, p, gain, l, weight, columns):
        sums = []
        for i, group in enumerate(groups):
            if i:
                recv_half(p)
            ssq, hs = scaled(p, gain, l, group)
            sums.append(ssq)
            if i + 1 < len(groups):
                for c in range(0, columns, 512):
                    dg_v[i, :, c:c + 512] = sum(jnp.dot(h, weight[l, sp, c:c + 512], preferred_element_type=F32) for h, sp in hs)
        total = sum(sums)
        store_sums(n, total)
        send_sums(n)
        inv = lax.rsqrt(total / d_loc + EPS)
        factors = [jnp.where(total < jnp.inf, inv * jnp.sqrt(q / half + EPS), 0.0) for q in sums]

        def product(c, width):
            last = sum(jnp.dot(h, weight[l, sp, c:c + width], preferred_element_type=F32) for h, sp in hs)
            return sum(f * dg_v[i, :, c:c + width] for i, f in enumerate(factors[:-1])) + factors[-1] * last
        return product

    loads["hid"].wait()
    for j in range(2):
        xh[0, j] = hid_v[:, j * half:(j + 1) * half]
    key_lane = lax.broadcasted_iota(jnp.int32, (cells, kl), 1)
    key_row = lax.broadcasted_iota(jnp.int32, (cells, kl), 0)
    group_row = lax.broadcasted_iota(jnp.int32, (16, 1), 0) // heads
    per_group = 16 // heads

    def prepare_rel(l):
        pr = lax.broadcasted_iota(jnp.int32, (kl, kl), 0)
        pc = lax.broadcasted_iota(jnp.int32, (kl, kl), 1)
        flip = (pc == (seq - 1 - pr // heads) * heads + lax.rem(pr, heads)).astype(F32).astype(BF16)
        relf_v[l] = jnp.dot(flip, rel_v[l], preferred_element_type=F32).astype(BF16)
        first = rel_v[l, 0:16].astype(F32)
        for h in range(heads):
            r0_v[l, pl.ds(h, rb, stride=heads), :] = jnp.broadcast_to(first[h:h + 1], (rb, hd))

    def merge(l, new, tile_s, cache):
        for i in range(per_group):
            for h in range(heads):
                tile_s[pl.ds(i * heads + h, rb, stride=16), :] = new[:, h * hd:(h + 1) * hd]
        for b in range(rb):
            tile = tile_s[16 * b:16 * b + 16].astype(BF16)
            at = lent_s[16 * b:16 * b + 16].astype(BF16)
            full = jnp.broadcast_to(tile[None], (kl // 16, 16, hd)).reshape(kl, hd)
            where_at = jnp.broadcast_to(at[None], (kl // 16, 16, hd)).reshape(kl, hd)
            cache[l, b] = jnp.where(pos_v[...] == where_at, full, cache[l, b])

    def prepare_lengths():
        pos_v[...] = (lax.broadcasted_iota(jnp.int32, (kl, hd), 0) // heads).astype(F32).astype(BF16)
        index = my * rb + lax.broadcasted_iota(jnp.int32, (16 * rb, rows), 0) // 16
        lent_s[...] = jnp.broadcast_to(to_column(len_v[...].astype(F32), index), (16 * rb, hd))

    def early_relayout(l, j):
        loads["w", l, j].wait()
        relayout(l, j)

    fills = {}
    if layers > 1:
        fills = {"q": lambda l: early_relayout(l, 0), "up": lambda l: early_relayout(l, 1), "rs": lambda l: early_relayout(l, 2), "rs2": prepare_rel}

    def fill_for(name, l):
        return None if l >= layers or name not in fills else (lambda: fills[name](l))

    for l in range(layers):
        p = 2 * l
        def send_qkv(j):
            for d in y_order:
                peer = lax.rem(my + d, ny)
                rows_at = pl.multiple_of(peer * rb, rb)
                send(qkv_tx.at[l, j, pl.ds(rows_at, rb)], qkv_rx.at[l, my, j], qkv_ss.at[l, j, peer], qkv_rs.at[l, j, my], {"y": peer})

        if l == 0:
            loads["na"].wait()
            norm_stage(p, p, na_v[l:l + 1])
            for j in range(3):
                early_relayout(0, j)
                qkv_tx[l, j] = jnp.dot(h_v[...], wqkv_v[l, :, j * hh:(j + 1) * hh], preferred_element_type=F32).astype(BF16)
                if j == 1:
                    pl.semaphore_wait(barrier, ny - 1 + chips)
                    send_sums(p)
                    send_qkv(0)
                if j:
                    send_qkv(j)
        else:
            product = gather_matmul(p, p - 1, na_v, l, wqkv_v, 3 * hh)
            for j in range(3):
                qkv_tx[l, j] = product(j * hh, hh).astype(BF16)
                send_qkv(j)
        own_at = pl.multiple_of(my * rb, rb)
        for j in range(3):
            qkv_rx[l, my, j] = qkv_tx[l, j, pl.ds(own_at, rb), :]
        if l == 0:
            for name in ("len", "rel", "bu", "bw", "nm"):
                loads[name].wait()
            prepare_rel(0)
        loads["k", l].wait()
        loads["v", l].wait()
        lens_row = len_v[...].astype(F32)
        want = my * rb + lax.broadcasted_iota(jnp.int32, (cells, rows), 0) // heads
        lens = to_column(lens_row, want).astype(jnp.int32)
        ratios = ratio_rows(2 * l)
        want16 = my * rb + lax.broadcasted_iota(jnp.int32, (rb, 128), 0)
        cols = [to_column(r, want16) for r in ratios]

        def gathered(j):
            for d in y_order:
                src = lax.rem(my + d, ny)
                recv(qkv_rx.at[l, src, j], qkv_ss.at[l, j, src], qkv_rs.at[l, j, src], {"y": src})
            tot = qkv_rx[l, 0, j].astype(F32) * cols[0]
            for s in range(1, ny):
                tot = tot + qkv_rx[l, s, j].astype(F32) * cols[s]
            return tot.astype(BF16).astype(F32)

        q = gathered(0)
        for h in range(heads):
            qh = q[:, h * hd:(h + 1) * hd]
            a_s[pl.ds(h, rb, stride=heads), :] = qh + bu_v[l, h:h + 1].astype(F32)
            c_s[pl.ds(h, rb, stride=heads), :] = qh + bw_v[l, h:h + 1].astype(F32)
        a = a_s[...].astype(BF16)
        c = c_s[...].astype(BF16)
        rel = lax.dot_general(c, relf_v[l], (((1,), (1,)), ((), ())), preferred_element_type=F32)
        shift = seq - 1 - lens
        bit = 1
        while bit < seq:
            rolled = pltpu.roll(rel, kl - bit * heads, 1)
            rel = jnp.where(lax.rem(shift // bit, 2) == 1, rolled, rel)
            bit *= 2
        score_parts = []
        for g in range(cells // 16):
            ag = a[16 * g:16 * g + 16]
            sg = None
            for i in range(per_group):
                o = lax.dot_general(ag, kc_v[l, g * per_group + i], (((1,), (1,)), ((), ())), preferred_element_type=F32)
                sg = o if sg is None else jnp.where(group_row == i, o, sg)
            score_parts.append(sg)
        scores = jnp.concatenate(score_parts, axis=0)
        k = gathered(1)
        v = gathered(2)
        for h in range(heads):
            k_s[pl.ds(h, rb, stride=heads), :] = k[:, h * hd:(h + 1) * hd]
            v_s[pl.ds(h, rb, stride=heads), :] = v[:, h * hd:(h + 1) * hd]
        kn = k_s[...]
        vn = v_s[...]
        scale = hd ** -0.5
        s_new = (jnp.sum(a.astype(F32) * kn, axis=1, keepdims=True) + jnp.sum(c.astype(F32) * r0_v[l], axis=1, keepdims=True)) * scale
        valid = (lax.rem(key_lane, heads) == lax.rem(key_row, heads)) & (key_lane // heads < lens)
        scores = jnp.where(valid, (scores + rel) * scale, -jnp.inf)
        top = jnp.maximum(jnp.max(scores, axis=1, keepdims=True), s_new)
        e = jnp.exp(scores - top)
        e_new = jnp.exp(s_new - top)
        inv_den = 1.0 / (jnp.sum(e, axis=1, keepdims=True) + e_new)
        prob = (e * inv_den).astype(BF16)
        p_new = (e_new * inv_den).astype(BF16).astype(F32)
        ctx_parts = []
        for g in range(cells // 16):
            pg = prob[16 * g:16 * g + 16]
            cg = None
            for i in range(0, per_group, 2):
                b = g * per_group + i
                values = jnp.concatenate([vc_v[l, b], vc_v[l, b + 1]], axis=1)
                o = jnp.dot(pg, values, preferred_element_type=F32)
                cg = o[:, :hd] if cg is None else jnp.where(group_row == i, o[:, :hd], cg)
                cg = jnp.where(group_row == i + 1, o[:, hd:], cg)
            ctx_parts.append(cg)
        ctx_s[...] = jnp.concatenate(ctx_parts, axis=0) + p_new * vn
        for h in range(heads):
            ctx_all[l, my, :, h * hd:(h + 1) * hd] = ctx_s[pl.ds(h, rb, stride=heads), :].astype(BF16)
        for d in y_order:
            peer = lax.rem(my + d, ny)
            send(ctx_all.at[l, my], ctx_all.at[l, my], ctx_ss.at[l, peer], ctx_rs.at[l, my], {"y": peer})
        if l == 0:
            prepare_lengths()
        if fill_for("q", l + 1) is not None:
            fills["q"](l + 1)
        merge(l, k, kt_s, kc_v)
        merge(l, v, vt_s, vc_v)
        loads["o", l].wait()
        for d in reversed(y_order):
            src = lax.rem(my + d, ny)
            recv(ctx_all.at[l, src], ctx_ss.at[l, src], ctx_rs.at[l, src], {"y": src})
        ctx = jnp.concatenate([ctx_all[l, s] for s in range(ny)], axis=0)
        x_reduce(p, lambda at: jnp.dot(ctx, wo_v[l, :, at], preferred_element_type=F32), fill_for("rs", l + 1))
        p = 2 * l + 1
        loads["up", l].wait()
        product = gather_matmul(p, p - 1, nm_v, l, wup_v, ff_loc)
        for hf in range(2):
            for j in range(ny):
                up_tx[l, hf, j] = product(j * fb + hf * fh, fh).astype(BF16)
            for d in y_order:
                dst = lax.rem(my + d, ny)
                send(up_tx.at[l, hf, dst], up_rx.at[l, hf, my], up_ss.at[l, hf, dst], up_rs.at[l, hf, my], {"y": dst})
        for hf in range(2):
            up_rx[l, hf, my] = up_tx[l, hf, my]
        if fill_for("up", l + 1) is not None:
            fills["up"](l + 1)
        ratios = ratio_rows(p)
        cols = [to_column(r, rown) for r in ratios]
        loads["dn", l].wait()
        for hf in range(2):
            for d in reversed(y_order):
                src = lax.rem(my + d, ny)
                recv(up_rx.at[l, hf, src], up_ss.at[l, hf, src], up_rs.at[l, hf, src], {"y": src})
            tot = up_rx[l, hf, 0].astype(F32) * cols[0]
            for s in range(1, ny):
                tot = tot + up_rx[l, hf, s].astype(F32) * cols[s]
            act[l, hf, my] = jax.nn.gelu(tot.astype(BF16).astype(F32), approximate=True).astype(BF16)
            for d in y_order:
                peer = lax.rem(my + d, ny)
                send(act.at[l, hf, my], act.at[l, hf, my], act_ss.at[l, hf, peer], act_rs.at[l, hf, my], {"y": peer})

        def down(hf, src, at=slice(None)):
            return jnp.dot(act[l, hf, src], wdn_v[l, pl.ds(pl.multiple_of(src * fb + hf * fh, fh), fh), at], preferred_element_type=F32)

        acc_v[...] = down(0, my) + down(1, my)
        pieces = [(hf, d) for hf in range(2) for d in reversed(y_order)]
        for hf, d in pieces:
            src = lax.rem(my + d, ny)
            recv(act.at[l, hf, src], act_ss.at[l, hf, src], act_rs.at[l, hf, src], {"y": src})
            if (hf, d) != pieces[-1]:
                acc_v[...] += down(hf, src)
        x_reduce(p, lambda at: acc_v[:, at] + down(hf, src, at), fill_for("rs2", l + 1))
    recv_half(2 * layers - 1)

    last = 2 * layers
    for j in range(2):
        hid_out[:, j * half:(j + 1) * half] = xh[last, j]
    for c in sends:
        c.wait_send()


def write_kernel(hid_in, kc_in, vc_in, hid_out, kc_out, vc_out, sem):
    copies = [pltpu.make_async_copy(hid_in, hid_out, sem.at[0])]
    layers, rb = kc_in.shape[:2]
    half = rb // 2
    for src, dst in ((kc_in, kc_out), (vc_in, vc_out)):
        for l in range(layers):
            for b in range(0, rb, half):
                copies.append(pltpu.make_async_copy(src.at[l, pl.ds(b, half)], dst.at[l, pl.ds(b, half)], sem.at[len(copies)]))
    for c in copies:
        c.start()
    for c in copies:
        c.wait()


def solution(mesh):
    ny = mesh.shape["y"]
    nx = mesh.shape["x"]
    cache_spec = P(None, ("rep", "y"), None, "x", None)
    row_spec = P("rep", "y")
    proj_spec = P(None, "y", "x", None)
    head_spec = P(None, "x", None)
    in_specs = (row_spec, P("rep"), cache_spec, cache_spec, P(None, None, "x", None), P(None, "y"),
                proj_spec, proj_spec, proj_spec, head_spec, head_spec, P(None, "x", None, "y"),
                P(None, "y"), P(None, "y", "x"), P(None, "x", "y"))
    out_specs = (row_spec, cache_spec, cache_spec)

    def local_step(hidden, lengths, k_cache, v_cache, rel_table, norm_attn, w_q, w_k, w_v, bias_content, bias_pos, w_out, norm_mlp, w_up, w_down):
        layers, rb, seq, heads, hd = k_cache.shape
        rows, d_loc = hidden.shape
        ff_loc = w_up.shape[2]
        hh = heads * hd
        cells = rb * heads
        kl = seq * heads
        half = d_loc // 2
        fb = ff_loc // ny
        dims = (layers, ny, nx, rows, heads, hd, seq, d_loc, ff_loc)
        any_spec = pl.BlockSpec(memory_space=pl.ANY)
        vmem = pltpu.VMEM
        dma = pltpu.SemaphoreType.DMA
        scratch = [
            vmem((rows, d_loc), BF16), vmem((1, rows), jnp.int32),
            vmem((layers, kl, hd), BF16), vmem((layers, d_loc), BF16), vmem((layers, d_loc), BF16),
            vmem((layers, heads, hd), BF16), vmem((layers, heads, hd), BF16),
            vmem((layers, 3, d_loc * heads, hd), BF16), vmem((layers, d_loc, 3 * hh), BF16),
            vmem((layers, hh, d_loc), BF16), vmem((layers, d_loc, ff_loc), BF16), vmem((layers, ff_loc, d_loc), BF16),
            vmem((128 * heads, hd), F32), vmem((layers, kl, hd), BF16), vmem((layers, cells, hd), F32), vmem((rows, d_loc), BF16),
            vmem((cells, hd), F32), vmem((cells, hd), F32), vmem((cells, hd), F32), vmem((cells, hd), F32), vmem((cells, hd), F32),
            vmem((rows, d_loc), F32), vmem((kl, hd), BF16), vmem((16 * rb, hd), F32), vmem((16 * rb, hd), F32), vmem((16 * rb, hd), F32),
            vmem((1, rows, max(ff_loc, 3 * hh)), F32),
            vmem((2 * layers, ny, 8, 128), F32),
            vmem((layers, 3, rows, hh), BF16), vmem((layers, ny, 3, rb, hh), BF16), vmem((layers, ny, rb, hh), BF16),
            vmem((2 * layers, rows, half), BF16), vmem((2 * layers, rows, half), BF16), vmem((2 * layers, nx // 2, rows, half), BF16), vmem((2 * layers + 1, 2, rows, half), BF16),
            vmem((layers, 2, ny, rows, fb // 2), BF16), vmem((layers, 2, ny, rows, fb // 2), BF16), vmem((layers, 2, ny, rows, fb // 2), BF16),
            dma((7 + 8 * layers,)),
            dma((2 * layers, ny)), dma((2 * layers, ny)), dma((layers, 3, ny)), dma((layers, 3, ny)),
            dma((layers, ny)), dma((layers, ny)), dma((2 * layers,)), dma((2 * layers,)), dma((2 * layers, nx // 2)), dma((2 * layers, nx // 2)),
            dma((2 * layers,)), dma((2 * layers,)), dma((layers, 2, ny)), dma((layers, 2, ny)), dma((layers, 2, ny)), dma((layers, 2, ny)),
        ]
        cache_dims = (layers, rb, kl, hd)
        vmem_spec = pl.BlockSpec(memory_space=vmem)
        hid, k_new, v_new = pl.pallas_call(
            functools.partial(step_kernel, dims),
            out_shape=(vmem((rows, d_loc), BF16), vmem(cache_dims, BF16), vmem(cache_dims, BF16)),
            in_specs=[any_spec] * 15,
            out_specs=(vmem_spec,) * 3,
            scratch_shapes=scratch,
            compiler_params=pltpu.CompilerParams(collective_id=0, has_side_effects=True, vmem_limit_bytes=46 * 1024 * 1024),
            name="decode_step",
        )(hidden, lengths.reshape(1, rows), k_cache.reshape(layers, rb, kl, hd), v_cache.reshape(layers, rb, kl, hd),
          rel_table.reshape(layers, kl, hd), norm_attn,
          w_q.reshape(layers, d_loc * heads, hd), w_k.reshape(layers, d_loc * heads, hd), w_v.reshape(layers, d_loc * heads, hd),
          bias_content, bias_pos, w_out.reshape(layers, hh, d_loc), norm_mlp, w_up, w_down)

        flat = jax.ShapeDtypeStruct(cache_dims, BF16)
        hid, k_new, v_new = pl.pallas_call(
            write_kernel,
            out_shape=(jax.ShapeDtypeStruct((rows, d_loc), BF16), flat, flat),
            in_specs=[vmem_spec] * 3,
            out_specs=(any_spec,) * 3,
            scratch_shapes=[dma((1 + 4 * layers,))],
            compiler_params=pltpu.CompilerParams(vmem_limit_bytes=2 * 1024 * 1024),
            name="cache_write",
        )(hid, k_new, v_new)
        return hid, k_new.reshape(k_cache.shape), v_new.reshape(v_cache.shape)

    return jax.shard_map(local_step, mesh=mesh, in_specs=in_specs, out_specs=out_specs, check_vma=False)
```

```python
import functools

import jax
import jax.numpy as jnp
from jax import lax
from jax.experimental import pallas as pl
from jax.experimental.pallas import tpu as pltpu
from jax.sharding import PartitionSpec as P

EPS = 1e-6
F32 = jnp.float32
BF16 = jnp.bfloat16
MESH = pl.DeviceIdType.MESH


def step_kernel(dims, hidden_in, len_in, kc_in, vc_in, rel_in, na_in, wq_in, wk_in, wv_in, bu_in, bw_in, wo_in, nm_in, wup_in, wdn_in,
                hid_out, kc_v, vc_v,
                hid_v, len_v, rel_v, na_v, nm_v, bu_v, bw_v, wraw_v, wqkv_v, wo_v, wup_v, wdn_v,
                wtmp, relf_v, r0_v, h_v, a_s, c_s, k_s, v_s, ctx_s, acc_v, pos_v, lent_s, kt_s, vt_s, dg_v,
                ss_rx, qkv_tx, qkv_rx, ctx_all, dd_tx, dd_rx, bc, xh, up_tx, up_rx, act,
                ld_sem, ss_ss, ss_rs, qkv_ss, qkv_rs, ctx_ss, ctx_rs, dd_ss, dd_rs, bc_ss, bc_rs, xe_ss, xe_rs, up_ss, up_rs, act_ss, act_rs):
    layers, ny, nx, rows, heads, hd, seq, d_loc, ff_loc = dims
    d_total = d_loc * ny
    rb = rows // ny
    hh = heads * hd
    half = d_loc // 2
    fb = ff_loc // ny
    cells = rb * heads
    kl = seq * heads
    chips = nx // 2
    fw = fb // 2
    fh = fw // 2
    my = lax.axis_index("y")
    mx = lax.axis_index("x")
    my_chip = mx // 2
    core = lax.rem(mx, 2)
    other = 1 - core
    partner = {"x": 2 * my_chip + other}

    barrier = pltpu.get_barrier_semaphore()
    for d in range(1, ny):
        pl.semaphore_signal(barrier, inc=1, device_id={"y": lax.rem(my + d, ny)}, device_id_type=MESH)
    pl.semaphore_signal(barrier, inc=1, device_id=partner, device_id_type=MESH)
    for d in range(1, chips):
        pl.semaphore_signal(barrier, inc=1, device_id={"x": 2 * lax.rem(my_chip + d, chips) + core}, device_id_type=MESH)

    loads = {}

    def load(name, src, dst):
        c = pltpu.make_async_copy(src, dst, ld_sem.at[len(loads)])
        c.start()
        loads[name] = c

    load("hid", hidden_in, hid_v)
    load("na", na_in, na_v)
    for j, w in enumerate((wq_in, wk_in, wv_in)):
        load(("w", 0, j), w.at[0], wraw_v.at[0, j])
    load("len", len_in, len_v)
    load("rel", rel_in, rel_v)
    load("bu", bu_in, bu_v)
    load("bw", bw_in, bw_v)
    load("nm", nm_in, nm_v)
    load(("k", 0), kc_in.at[0], kc_v.at[0])
    load(("v", 0), vc_in.at[0], vc_v.at[0])
    load(("o", 0), wo_in.at[0], wo_v.at[0])
    load(("up", 0), wup_in.at[0], wup_v.at[0])
    load(("dn", 0), wdn_in.at[0], wdn_v.at[0])
    for l in range(1, layers):
        for j, w in enumerate((wq_in, wk_in, wv_in)):
            load(("w", l, j), w.at[l], wraw_v.at[l, j])
        load(("k", l), kc_in.at[l], kc_v.at[l])
        load(("v", l), vc_in.at[l], vc_v.at[l])
        load(("o", l), wo_in.at[l], wo_v.at[l])
        load(("up", l), wup_in.at[l], wup_v.at[l])
        load(("dn", l), wdn_in.at[l], wdn_v.at[l])

    sends = []

    def send(src, dst, ss, rs, dev):
        c = pltpu.make_async_remote_copy(src_ref=src, dst_ref=dst, send_sem=ss, recv_sem=rs, device_id=dev, device_id_type=MESH)
        c.start()
        sends.append(c)

    def recv(dst, ss, rs, dev):
        pltpu.make_async_remote_copy(src_ref=dst, dst_ref=dst, send_sem=ss, recv_sem=rs, device_id=dev, device_id_type=MESH).wait_recv()

    chip_order = sorted(range(1, chips), key=lambda d: -min(d, chips - d))
    y_order = list(range(1, ny))
    down_order = sorted(y_order, key=lambda d: min(d, ny - d))
    chunk_k = 128
    chunk = chunk_k * heads

    def relayout(l, j):
        def body(i, carry):
            wtmp[...] = wraw_v[l, j, pl.ds(pl.multiple_of(i * chunk, chunk), chunk), :].astype(F32)
            for h in range(heads):
                wqkv_v[l, pl.ds(pl.multiple_of(i * chunk_k, chunk_k), chunk_k), j * hh + h * hd:j * hh + (h + 1) * hd] = wtmp[pl.ds(h, chunk_k, stride=heads), :].astype(BF16)
            return carry
        lax.fori_loop(0, d_loc // chunk_k, body, 0)

    lane = lax.broadcasted_iota(jnp.int32, (rows, 128), 1)
    rown = lax.broadcasted_iota(jnp.int32, (rows, 128), 0)
    diag = lane == rown

    def store_sums(n, ssq):
        row = jnp.sum(jnp.where(diag, ssq, 0.0), axis=0, keepdims=True)
        ss_rx[n, my] = jnp.broadcast_to(row, (8, 128))

    def norm_stage(n, p, gain):
        blocks = [xh[p, j].astype(F32) for j in range(2)]
        ssq = jnp.sum(sum(b * b for b in blocks), axis=1, keepdims=True)
        store_sums(n, ssq)
        inv = lax.rsqrt(ssq / d_loc + EPS)
        for j in range(2):
            h_v[:, j * half:(j + 1) * half] = (blocks[j] * inv * gain[:, j * half:(j + 1) * half].astype(F32)).astype(BF16)

    def send_sums(n):
        for d in y_order:
            peer = lax.rem(my + d, ny)
            send(ss_rx.at[n, my], ss_rx.at[n, my], ss_ss.at[n, peer], ss_rs.at[n, my], {"y": peer})

    def ratio_rows(n):
        for d in y_order:
            src = lax.rem(my + d, ny)
            recv(ss_rx.at[n, src], ss_ss.at[n, src], ss_rs.at[n, src], {"y": src})
        parts = [ss_rx[n, s][0:1] for s in range(ny)]
        total = parts[0]
        for s in range(1, ny):
            total = total + parts[s]
        inv = lax.rsqrt(total / d_total + EPS)
        finite = total < jnp.inf
        return [jnp.where(finite, inv * jnp.sqrt(parts[s] / d_loc + EPS), 0.0) for s in range(ny)]

    def to_column(row, index):
        return jnp.sum(jnp.where(lax.broadcasted_iota(jnp.int32, index.shape, 1) == index, row, 0.0), axis=1, keepdims=True)

    def half_at(which):
        return pl.ds(pl.multiple_of(which * half, half), half)

    def x_reduce(p, part, fill=None):
        dd_tx[p] = part(half_at(other)).astype(BF16)
        send(dd_tx.at[p], dd_rx.at[p], dd_ss.at[p], dd_rs.at[p], partner)
        own = part(half_at(core))
        recv(dd_rx.at[p], dd_ss.at[p], dd_rs.at[p], partner)
        bc[p, my_chip] = (own + dd_rx[p].astype(F32)).astype(BF16)
        for d in chip_order:
            chip = lax.rem(my_chip + d, chips)
            send(bc.at[p, my_chip], bc.at[p, my_chip], bc_ss.at[p, chip], bc_rs.at[p, my_chip], {"x": 2 * chip + core})
        if fill is not None:
            fill()
        for d in reversed(chip_order):
            chip = lax.rem(my_chip + d, chips)
            recv(bc.at[p, chip], bc_ss.at[p, chip], bc_rs.at[p, chip], {"x": 2 * chip + core})
        total = xh[p, core].astype(F32)
        for chip in range(chips):
            total = total + bc[p, chip].astype(F32)
        xh[p + 1, core] = total.astype(BF16)
        send(xh.at[p + 1, core], xh.at[p + 1, core], xe_ss.at[p], xe_rs.at[p], partner)

    def recv_half(p):
        recv(xh.at[p + 1, other], xe_ss.at[p], xe_rs.at[p], partner)

    groups = [core, other]

    def scaled(p, gain, l, which):
        block = xh[p + 1, which].astype(F32)
        ssq = jnp.sum(block * block, axis=1, keepdims=True)
        inv = lax.rsqrt(ssq / half + EPS)
        at = half_at(which)
        return ssq, [((block * inv * gain[l:l + 1, at].astype(F32)).astype(BF16), at)]

    def gather_matmul(n, p, gain, l, weight, columns):
        sums = []
        for i, group in enumerate(groups):
            if i:
                recv_half(p)
            ssq, hs = scaled(p, gain, l, group)
            sums.append(ssq)
            if i + 1 < len(groups):
                for c in range(0, columns, 512):
                    dg_v[i, :, c:c + 512] = sum(jnp.dot(h, weight[l, sp, c:c + 512], preferred_element_type=F32) for h, sp in hs)
        total = sum(sums)
        store_sums(n, total)
        send_sums(n)
        inv = lax.rsqrt(total / d_loc + EPS)
        factors = [jnp.where(total < jnp.inf, inv * jnp.sqrt(q / half + EPS), 0.0) for q in sums]

        def product(at):
            last = sum(jnp.dot(h, weight[l, sp, at], preferred_element_type=F32) for h, sp in hs)
            return sum(f * dg_v[i, :, at] for i, f in enumerate(factors[:-1])) + factors[-1] * last
        return product

    loads["hid"].wait()
    for j in range(2):
        xh[0, j] = hid_v[:, j * half:(j + 1) * half]
    key_lane = lax.broadcasted_iota(jnp.int32, (cells, kl), 1)
    key_row = lax.broadcasted_iota(jnp.int32, (cells, kl), 0)
    group_row = lax.broadcasted_iota(jnp.int32, (16, 1), 0) // heads
    per_group = 16 // heads

    def prepare_rel(l):
        pr = lax.broadcasted_iota(jnp.int32, (kl, kl), 0)
        pc = lax.broadcasted_iota(jnp.int32, (kl, kl), 1)
        flip = (pc == (seq - 1 - pr // heads) * heads + lax.rem(pr, heads)).astype(F32).astype(BF16)
        relf_v[l] = jnp.dot(flip, rel_v[l], preferred_element_type=F32).astype(BF16)
        first = rel_v[l, 0:16].astype(F32)
        for h in range(heads):
            r0_v[l, pl.ds(h, rb, stride=heads), :] = jnp.broadcast_to(first[h:h + 1], (rb, hd))

    def merge(l, new, tile_s, cache):
        for i in range(per_group):
            for h in range(heads):
                tile_s[pl.ds(i * heads + h, rb, stride=16), :] = new[:, h * hd:(h + 1) * hd]
        for b in range(rb):
            tile = tile_s[16 * b:16 * b + 16].astype(BF16)
            at = lent_s[16 * b:16 * b + 16].astype(BF16)
            full = jnp.broadcast_to(tile[None], (kl // 16, 16, hd)).reshape(kl, hd)
            where_at = jnp.broadcast_to(at[None], (kl // 16, 16, hd)).reshape(kl, hd)
            cache[l, b] = jnp.where(pos_v[...] == where_at, full, cache[l, b])

    def prepare_lengths():
        pos_v[...] = (lax.broadcasted_iota(jnp.int32, (kl, hd), 0) // heads).astype(F32).astype(BF16)
        index = my * rb + lax.broadcasted_iota(jnp.int32, (16 * rb, rows), 0) // 16
        lent_s[...] = jnp.broadcast_to(to_column(len_v[...].astype(F32), index), (16 * rb, hd))

    def early_relayout(l, j):
        loads["w", l, j].wait()
        relayout(l, j)

    fills = {}
    if layers > 1:
        fills = {"q": lambda l: early_relayout(l, 0), "up": lambda l: early_relayout(l, 1), "rs": lambda l: early_relayout(l, 2), "rs2": prepare_rel}

    def fill_for(name, l):
        return None if l >= layers or name not in fills else (lambda: fills[name](l))

    for l in range(layers):
        p = 2 * l
        def send_qkv(j):
            for d in y_order:
                peer = lax.rem(my + d, ny)
                rows_at = pl.multiple_of(peer * rb, rb)
                send(qkv_tx.at[l, j, pl.ds(rows_at, rb)], qkv_rx.at[l, my, j], qkv_ss.at[l, j, peer], qkv_rs.at[l, j, my], {"y": peer})

        if l == 0:
            loads["na"].wait()
            norm_stage(p, p, na_v[l:l + 1])
            for j in range(3):
                early_relayout(0, j)
                qkv_tx[l, j] = jnp.dot(h_v[...], wqkv_v[l, :, j * hh:(j + 1) * hh], preferred_element_type=F32).astype(BF16)
                if j == 1:
                    pl.semaphore_wait(barrier, ny - 1 + chips)
                    send_sums(p)
                    send_qkv(0)
                if j:
                    send_qkv(j)
        else:
            product = gather_matmul(p, p - 1, na_v, l, wqkv_v, 3 * hh)
            for j in range(3):
                qkv_tx[l, j] = product(slice(j * hh, (j + 1) * hh)).astype(BF16)
                send_qkv(j)
        own_at = pl.multiple_of(my * rb, rb)
        for j in range(3):
            qkv_rx[l, my, j] = qkv_tx[l, j, pl.ds(own_at, rb), :]
        if l == 0:
            for name in ("len", "rel", "bu", "bw", "nm"):
                loads[name].wait()
            prepare_rel(0)
        loads["k", l].wait()
        loads["v", l].wait()
        lens_row = len_v[...].astype(F32)
        want = my * rb + lax.broadcasted_iota(jnp.int32, (cells, rows), 0) // heads
        lens = to_column(lens_row, want).astype(jnp.int32)
        ratios = ratio_rows(2 * l)
        want16 = my * rb + lax.broadcasted_iota(jnp.int32, (rb, 128), 0)
        cols = [to_column(r, want16) for r in ratios]

        def gathered(j):
            for d in y_order:
                src = lax.rem(my + d, ny)
                recv(qkv_rx.at[l, src, j], qkv_ss.at[l, j, src], qkv_rs.at[l, j, src], {"y": src})
            tot = qkv_rx[l, 0, j].astype(F32) * cols[0]
            for s in range(1, ny):
                tot = tot + qkv_rx[l, s, j].astype(F32) * cols[s]
            return tot.astype(BF16).astype(F32)

        q = gathered(0)
        for h in range(heads):
            qh = q[:, h * hd:(h + 1) * hd]
            a_s[pl.ds(h, rb, stride=heads), :] = qh + bu_v[l, h:h + 1].astype(F32)
            c_s[pl.ds(h, rb, stride=heads), :] = qh + bw_v[l, h:h + 1].astype(F32)
        a = a_s[...].astype(BF16)
        c = c_s[...].astype(BF16)
        rel = lax.dot_general(c, relf_v[l], (((1,), (1,)), ((), ())), preferred_element_type=F32)
        shift = seq - 1 - lens
        unit = 1
        while unit < seq:
            digit = lax.rem(shift // unit, 4)
            rolled = rel
            for m in range(1, 4):
                if m * unit < seq:
                    rolled = jnp.where(digit == m, pltpu.roll(rel, kl - m * unit * heads, 1), rolled)
            rel = rolled
            unit *= 4
        score_parts = []
        for g in range(cells // 16):
            ag = a[16 * g:16 * g + 16]
            sg = None
            for i in range(per_group):
                o = lax.dot_general(ag, kc_v[l, g * per_group + i], (((1,), (1,)), ((), ())), preferred_element_type=F32)
                sg = o if sg is None else jnp.where(group_row == i, o, sg)
            score_parts.append(sg)
        scores = jnp.concatenate(score_parts, axis=0)
        k = gathered(1)
        v = gathered(2)
        for h in range(heads):
            k_s[pl.ds(h, rb, stride=heads), :] = k[:, h * hd:(h + 1) * hd]
            v_s[pl.ds(h, rb, stride=heads), :] = v[:, h * hd:(h + 1) * hd]
        kn = k_s[...]
        vn = v_s[...]
        scale = hd ** -0.5
        s_new = (jnp.sum(a.astype(F32) * kn, axis=1, keepdims=True) + jnp.sum(c.astype(F32) * r0_v[l], axis=1, keepdims=True)) * scale
        valid = (lax.rem(key_lane, heads) == lax.rem(key_row, heads)) & (key_lane // heads < lens)
        scores = jnp.where(valid, (scores + rel) * scale, -jnp.inf)
        top = jnp.maximum(jnp.max(scores, axis=1, keepdims=True), s_new)
        e = jnp.exp(scores - top)
        e_new = jnp.exp(s_new - top)
        inv_den = 1.0 / (jnp.sum(e, axis=1, keepdims=True) + e_new)
        prob = (e * inv_den).astype(BF16)
        p_new = (e_new * inv_den).astype(BF16).astype(F32)
        ctx_parts = []
        for g in range(cells // 16):
            pg = prob[16 * g:16 * g + 16]
            cg = None
            for i in range(0, per_group, 2):
                b = g * per_group + i
                values = jnp.concatenate([vc_v[l, b], vc_v[l, b + 1]], axis=1)
                o = jnp.dot(pg, values, preferred_element_type=F32)
                cg = o[:, :hd] if cg is None else jnp.where(group_row == i, o[:, :hd], cg)
                cg = jnp.where(group_row == i + 1, o[:, hd:], cg)
            ctx_parts.append(cg)
        ctx_s[...] = jnp.concatenate(ctx_parts, axis=0) + p_new * vn
        for h in range(heads):
            ctx_all[l, my, :, h * hd:(h + 1) * hd] = ctx_s[pl.ds(h, rb, stride=heads), :].astype(BF16)
        for d in y_order:
            peer = lax.rem(my + d, ny)
            send(ctx_all.at[l, my], ctx_all.at[l, my], ctx_ss.at[l, peer], ctx_rs.at[l, my], {"y": peer})
        if l == 0:
            prepare_lengths()
        if fill_for("q", l + 1) is not None:
            fills["q"](l + 1)
        merge(l, k, kt_s, kc_v)
        merge(l, v, vt_s, vc_v)
        loads["o", l].wait()
        for d in reversed(y_order):
            src = lax.rem(my + d, ny)
            recv(ctx_all.at[l, src], ctx_ss.at[l, src], ctx_rs.at[l, src], {"y": src})
        ctx = jnp.concatenate([ctx_all[l, s] for s in range(ny)], axis=0)
        x_reduce(p, lambda at: jnp.dot(ctx, wo_v[l, :, at], preferred_element_type=F32), fill_for("rs", l + 1))
        p = 2 * l + 1
        loads["up", l].wait()
        product = gather_matmul(p, p - 1, nm_v, l, wup_v, ff_loc)
        def up_blocks(w, dst, to):
            block = product(pl.ds(pl.multiple_of(dst * fb + w * fw, fw), fw)).astype(BF16)
            for i in range(2):
                to[l, 2 * w + i, dst] = block[:, i * fh:(i + 1) * fh]

        for w in range(2):
            for d in y_order:
                up_blocks(w, lax.rem(my + d, ny), up_tx)
            for hf in (2 * w, 2 * w + 1):
                for d in y_order:
                    dst = lax.rem(my + d, ny)
                    send(up_tx.at[l, hf, dst], up_rx.at[l, hf, my], up_ss.at[l, hf, dst], up_rs.at[l, hf, my], {"y": dst})
        for w in range(2):
            up_blocks(w, my, up_rx)
        if fill_for("up", l + 1) is not None:
            fills["up"](l + 1)
        ratios = ratio_rows(p)
        cols = [to_column(r, rown) for r in ratios]
        loads["dn", l].wait()
        for hf in range(4):
            for d in reversed(y_order):
                src = lax.rem(my + d, ny)
                recv(up_rx.at[l, hf, src], up_ss.at[l, hf, src], up_rs.at[l, hf, src], {"y": src})
            tot = up_rx[l, hf, 0].astype(F32) * cols[0]
            for s in range(1, ny):
                tot = tot + up_rx[l, hf, s].astype(F32) * cols[s]
            act[l, hf, my] = jax.nn.gelu(tot.astype(BF16).astype(F32), approximate=True).astype(BF16)
            for d in y_order:
                peer = lax.rem(my + d, ny)
                send(act.at[l, hf, my], act.at[l, hf, my], act_ss.at[l, hf, peer], act_rs.at[l, hf, my], {"y": peer})

        def down(w, src, at=slice(None)):
            pieces = jnp.concatenate([act[l, 2 * w, src], act[l, 2 * w + 1, src]], axis=1)
            return jnp.dot(pieces, wdn_v[l, pl.ds(pl.multiple_of(src * fb + w * fw, fw), fw), at], preferred_element_type=F32)

        acc_v[...] = down(0, my) + down(1, my)
        steps = [(w, d) for w in range(2) for d in down_order]
        for w, d in steps:
            src = lax.rem(my + d, ny)
            for hf in (2 * w, 2 * w + 1):
                recv(act.at[l, hf, src], act_ss.at[l, hf, src], act_rs.at[l, hf, src], {"y": src})
            if (w, d) != steps[-1]:
                acc_v[...] += down(w, src)
        x_reduce(p, lambda at: acc_v[:, at] + down(w, src, at), fill_for("rs2", l + 1))
    recv_half(2 * layers - 1)

    last = 2 * layers
    for j in range(2):
        hid_out[:, j * half:(j + 1) * half] = xh[last, j]
    for c in sends:
        c.wait_send()


def write_kernel(hid_in, kc_in, vc_in, hid_out, kc_out, vc_out, sem):
    copies = [pltpu.make_async_copy(hid_in, hid_out, sem.at[0])]
    layers, rb = kc_in.shape[:2]
    half = rb // 2
    for src, dst in ((kc_in, kc_out), (vc_in, vc_out)):
        for l in range(layers):
            for b in range(0, rb, half):
                copies.append(pltpu.make_async_copy(src.at[l, pl.ds(b, half)], dst.at[l, pl.ds(b, half)], sem.at[len(copies)]))
    for c in copies:
        c.start()
    for c in copies:
        c.wait()


def solution(mesh):
    ny = mesh.shape["y"]
    nx = mesh.shape["x"]
    cache_spec = P(None, ("rep", "y"), None, "x", None)
    row_spec = P("rep", "y")
    proj_spec = P(None, "y", "x", None)
    head_spec = P(None, "x", None)
    in_specs = (row_spec, P("rep"), cache_spec, cache_spec, P(None, None, "x", None), P(None, "y"),
                proj_spec, proj_spec, proj_spec, head_spec, head_spec, P(None, "x", None, "y"),
                P(None, "y"), P(None, "y", "x"), P(None, "x", "y"))
    out_specs = (row_spec, cache_spec, cache_spec)

    def local_step(hidden, lengths, k_cache, v_cache, rel_table, norm_attn, w_q, w_k, w_v, bias_content, bias_pos, w_out, norm_mlp, w_up, w_down):
        layers, rb, seq, heads, hd = k_cache.shape
        rows, d_loc = hidden.shape
        ff_loc = w_up.shape[2]
        hh = heads * hd
        cells = rb * heads
        kl = seq * heads
        half = d_loc // 2
        fb = ff_loc // ny
        dims = (layers, ny, nx, rows, heads, hd, seq, d_loc, ff_loc)
        any_spec = pl.BlockSpec(memory_space=pl.ANY)
        vmem = pltpu.VMEM
        dma = pltpu.SemaphoreType.DMA
        scratch = [
            vmem((rows, d_loc), BF16), vmem((1, rows), jnp.int32),
            vmem((layers, kl, hd), BF16), vmem((layers, d_loc), BF16), vmem((layers, d_loc), BF16),
            vmem((layers, heads, hd), BF16), vmem((layers, heads, hd), BF16),
            vmem((layers, 3, d_loc * heads, hd), BF16), vmem((layers, d_loc, 3 * hh), BF16),
            vmem((layers, hh, d_loc), BF16), vmem((layers, d_loc, ff_loc), BF16), vmem((layers, ff_loc, d_loc), BF16),
            vmem((128 * heads, hd), F32), vmem((layers, kl, hd), BF16), vmem((layers, cells, hd), F32), vmem((rows, d_loc), BF16),
            vmem((cells, hd), F32), vmem((cells, hd), F32), vmem((cells, hd), F32), vmem((cells, hd), F32), vmem((cells, hd), F32),
            vmem((rows, d_loc), F32), vmem((kl, hd), BF16), vmem((16 * rb, hd), F32), vmem((16 * rb, hd), F32), vmem((16 * rb, hd), F32),
            vmem((1, rows, max(ff_loc, 3 * hh)), F32),
            vmem((2 * layers, ny, 8, 128), F32),
            vmem((layers, 3, rows, hh), BF16), vmem((layers, ny, 3, rb, hh), BF16), vmem((layers, ny, rb, hh), BF16),
            vmem((2 * layers, rows, half), BF16), vmem((2 * layers, rows, half), BF16), vmem((2 * layers, nx // 2, rows, half), BF16), vmem((2 * layers + 1, 2, rows, half), BF16),
            vmem((layers, 4, ny, rows, fb // 4), BF16), vmem((layers, 4, ny, rows, fb // 4), BF16), vmem((layers, 4, ny, rows, fb // 4), BF16),
            dma((7 + 8 * layers,)),
            dma((2 * layers, ny)), dma((2 * layers, ny)), dma((layers, 3, ny)), dma((layers, 3, ny)),
            dma((layers, ny)), dma((layers, ny)), dma((2 * layers,)), dma((2 * layers,)), dma((2 * layers, nx // 2)), dma((2 * layers, nx // 2)),
            dma((2 * layers,)), dma((2 * layers,)), dma((layers, 4, ny)), dma((layers, 4, ny)), dma((layers, 4, ny)), dma((layers, 4, ny)),
        ]
        cache_dims = (layers, rb, kl, hd)
        vmem_spec = pl.BlockSpec(memory_space=vmem)
        hid, k_new, v_new = pl.pallas_call(
            functools.partial(step_kernel, dims),
            out_shape=(vmem((rows, d_loc), BF16), vmem(cache_dims, BF16), vmem(cache_dims, BF16)),
            in_specs=[any_spec] * 15,
            out_specs=(vmem_spec,) * 3,
            scratch_shapes=scratch,
            compiler_params=pltpu.CompilerParams(collective_id=0, has_side_effects=True, vmem_limit_bytes=46 * 1024 * 1024),
            name="decode_step",
        )(hidden, lengths.reshape(1, rows), k_cache.reshape(layers, rb, kl, hd), v_cache.reshape(layers, rb, kl, hd),
          rel_table.reshape(layers, kl, hd), norm_attn,
          w_q.reshape(layers, d_loc * heads, hd), w_k.reshape(layers, d_loc * heads, hd), w_v.reshape(layers, d_loc * heads, hd),
          bias_content, bias_pos, w_out.reshape(layers, hh, d_loc), norm_mlp, w_up, w_down)

        flat = jax.ShapeDtypeStruct(cache_dims, BF16)
        hid, k_new, v_new = pl.pallas_call(
            write_kernel,
            out_shape=(jax.ShapeDtypeStruct((rows, d_loc), BF16), flat, flat),
            in_specs=[vmem_spec] * 3,
            out_specs=(any_spec,) * 3,
            scratch_shapes=[dma((1 + 4 * layers,))],
            compiler_params=pltpu.CompilerParams(vmem_limit_bytes=2 * 1024 * 1024),
            name="cache_write",
        )(hid, k_new, v_new)
        return hid, k_new.reshape(k_cache.shape), v_new.reshape(v_cache.shape)

    return jax.shard_map(local_step, mesh=mesh, in_specs=in_specs, out_specs=out_specs, check_vma=False)
```

```python
import functools

import jax
import jax.numpy as jnp
from jax import lax
from jax.experimental import pallas as pl
from jax.experimental.pallas import tpu as pltpu
from jax.sharding import PartitionSpec as P

EPS = 1e-6
F32 = jnp.float32
BF16 = jnp.bfloat16
MESH = pl.DeviceIdType.MESH


def step_kernel(dims, hidden_in, len_in, kc_in, vc_in, rel_in, na_in, wq_in, wk_in, wv_in, bu_in, bw_in, wo_in, nm_in, wup_in, wdn_in,
                hid_out, kc_v, vc_v,
                hid_v, len_v, rel_v, na_v, nm_v, bu_v, bw_v, wraw_v, wqkv_v, wo_v, wup_v, wdn_v,
                wtmp, relf_v, r0_v, h_v, a_s, c_s, k_s, v_s, ctx_s, acc_v, pos_v, lent_s, kt_s, vt_s, dg_v,
                ss_rx, qkv_tx, qkv_rx, ctx_all, dd_tx, dd_rx, bc, xh, up_tx, up_rx, act,
                ld_sem, ss_ss, ss_rs, qkv_ss, qkv_rs, ctx_ss, ctx_rs, dd_ss, dd_rs, bc_ss, bc_rs, xe_ss, xe_rs, up_ss, up_rs, act_ss, act_rs):
    layers, ny, nx, rows, heads, hd, seq, d_loc, ff_loc = dims
    d_total = d_loc * ny
    rb = rows // ny
    hh = heads * hd
    half = d_loc // 2
    fb = ff_loc // ny
    cells = rb * heads
    kl = seq * heads
    chips = nx // 2
    fw = fb // 2
    fh = fw // 2
    my = lax.axis_index("y")
    mx = lax.axis_index("x")
    my_chip = mx // 2
    core = lax.rem(mx, 2)
    other = 1 - core
    partner = {"x": 2 * my_chip + other}

    barrier = pltpu.get_barrier_semaphore()
    for d in range(1, ny):
        pl.semaphore_signal(barrier, inc=1, device_id={"y": lax.rem(my + d, ny)}, device_id_type=MESH)
    pl.semaphore_signal(barrier, inc=1, device_id=partner, device_id_type=MESH)
    for d in range(1, chips):
        pl.semaphore_signal(barrier, inc=1, device_id={"x": 2 * lax.rem(my_chip + d, chips) + core}, device_id_type=MESH)

    loads = {}

    def load(name, src, dst):
        c = pltpu.make_async_copy(src, dst, ld_sem.at[len(loads)])
        c.start()
        loads[name] = c

    load("hid", hidden_in, hid_v)
    load("na", na_in, na_v)
    for j, w in enumerate((wq_in, wk_in, wv_in)):
        load(("w", 0, j), w.at[0], wraw_v.at[0, j])
    load("len", len_in, len_v)
    load("rel", rel_in, rel_v)
    load("bu", bu_in, bu_v)
    load("bw", bw_in, bw_v)
    load("nm", nm_in, nm_v)
    load(("k", 0), kc_in.at[0], kc_v.at[0])
    load(("v", 0), vc_in.at[0], vc_v.at[0])
    load(("o", 0), wo_in.at[0], wo_v.at[0])
    load(("up", 0), wup_in.at[0], wup_v.at[0])
    load(("dn", 0), wdn_in.at[0], wdn_v.at[0])
    for l in range(1, layers):
        for j, w in enumerate((wq_in, wk_in, wv_in)):
            load(("w", l, j), w.at[l], wraw_v.at[l, j])
        load(("k", l), kc_in.at[l], kc_v.at[l])
        load(("v", l), vc_in.at[l], vc_v.at[l])
        load(("o", l), wo_in.at[l], wo_v.at[l])
        load(("up", l), wup_in.at[l], wup_v.at[l])
        load(("dn", l), wdn_in.at[l], wdn_v.at[l])

    sends = []

    def send(src, dst, ss, rs, dev):
        c = pltpu.make_async_remote_copy(src_ref=src, dst_ref=dst, send_sem=ss, recv_sem=rs, device_id=dev, device_id_type=MESH)
        c.start()
        sends.append(c)

    def recv(dst, ss, rs, dev):
        pltpu.make_async_remote_copy(src_ref=dst, dst_ref=dst, send_sem=ss, recv_sem=rs, device_id=dev, device_id_type=MESH).wait_recv()

    chip_order = sorted(range(1, chips), key=lambda d: -min(d, chips - d))
    y_order = list(range(1, ny))
    down_order = sorted(y_order, key=lambda d: min(d, ny - d))
    chunk_k = 128
    chunk = chunk_k * heads

    def relayout(l, j):
        def body(i, carry):
            wtmp[...] = wraw_v[l, j, pl.ds(pl.multiple_of(i * chunk, chunk), chunk), :].astype(F32)
            for h in range(heads):
                wqkv_v[l, pl.ds(pl.multiple_of(i * chunk_k, chunk_k), chunk_k), j * hh + h * hd:j * hh + (h + 1) * hd] = wtmp[pl.ds(h, chunk_k, stride=heads), :].astype(BF16)
            return carry
        lax.fori_loop(0, d_loc // chunk_k, body, 0)

    lane = lax.broadcasted_iota(jnp.int32, (rows, 128), 1)
    rown = lax.broadcasted_iota(jnp.int32, (rows, 128), 0)
    diag = lane == rown

    def store_sums(n, ssq):
        row = jnp.sum(jnp.where(diag, ssq, 0.0), axis=0, keepdims=True)
        ss_rx[n, my] = jnp.broadcast_to(row, (8, 128))

    def norm_stage(n, p, gain):
        blocks = [xh[p, j].astype(F32) for j in range(2)]
        ssq = jnp.sum(sum(b * b for b in blocks), axis=1, keepdims=True)
        store_sums(n, ssq)
        inv = lax.rsqrt(ssq / d_loc + EPS)
        for j in range(2):
            h_v[:, j * half:(j + 1) * half] = (blocks[j] * inv * gain[:, j * half:(j + 1) * half].astype(F32)).astype(BF16)

    def send_sums(n):
        for d in y_order:
            peer = lax.rem(my + d, ny)
            send(ss_rx.at[n, my], ss_rx.at[n, my], ss_ss.at[n, peer], ss_rs.at[n, my], {"y": peer})

    def ratio_rows(n):
        for d in y_order:
            src = lax.rem(my + d, ny)
            recv(ss_rx.at[n, src], ss_ss.at[n, src], ss_rs.at[n, src], {"y": src})
        parts = [ss_rx[n, s][0:1] for s in range(ny)]
        total = parts[0]
        for s in range(1, ny):
            total = total + parts[s]
        inv = lax.rsqrt(total / d_total + EPS)
        finite = total < jnp.inf
        return [jnp.where(finite, inv * jnp.sqrt(parts[s] / d_loc + EPS), 0.0) for s in range(ny)]

    def to_column(row, index):
        return jnp.sum(jnp.where(lax.broadcasted_iota(jnp.int32, index.shape, 1) == index, row, 0.0), axis=1, keepdims=True)

    def half_at(which):
        return pl.ds(pl.multiple_of(which * half, half), half)

    def x_reduce(p, part, fill=None):
        dd_tx[p] = part(half_at(other)).astype(BF16)
        send(dd_tx.at[p], dd_rx.at[p], dd_ss.at[p], dd_rs.at[p], partner)
        own = part(half_at(core))
        recv(dd_rx.at[p], dd_ss.at[p], dd_rs.at[p], partner)
        bc[p, my_chip] = (own + dd_rx[p].astype(F32)).astype(BF16)
        for d in chip_order:
            chip = lax.rem(my_chip + d, chips)
            send(bc.at[p, my_chip], bc.at[p, my_chip], bc_ss.at[p, chip], bc_rs.at[p, my_chip], {"x": 2 * chip + core})
        if fill is not None:
            fill()
        for d in reversed(chip_order):
            chip = lax.rem(my_chip + d, chips)
            recv(bc.at[p, chip], bc_ss.at[p, chip], bc_rs.at[p, chip], {"x": 2 * chip + core})
        total = xh[p, core].astype(F32)
        for chip in range(chips):
            total = total + bc[p, chip].astype(F32)
        xh[p + 1, core] = total.astype(BF16)
        send(xh.at[p + 1, core], xh.at[p + 1, core], xe_ss.at[p], xe_rs.at[p], partner)

    def recv_half(p):
        recv(xh.at[p + 1, other], xe_ss.at[p], xe_rs.at[p], partner)

    groups = [core, other]

    def scaled(p, gain, l, which):
        block = xh[p + 1, which].astype(F32)
        ssq = jnp.sum(block * block, axis=1, keepdims=True)
        inv = lax.rsqrt(ssq / half + EPS)
        at = half_at(which)
        return ssq, [((block * inv * gain[l:l + 1, at].astype(F32)).astype(BF16), at)]

    def gather_matmul(n, p, gain, l, weight, columns):
        sums = []
        for i, group in enumerate(groups):
            if i:
                recv_half(p)
            ssq, hs = scaled(p, gain, l, group)
            sums.append(ssq)
            if i + 1 < len(groups):
                for c in range(0, columns, 512):
                    dg_v[i, :, c:c + 512] = sum(jnp.dot(h, weight[l, sp, c:c + 512], preferred_element_type=F32) for h, sp in hs)
        total = sum(sums)
        store_sums(n, total)
        send_sums(n)
        inv = lax.rsqrt(total / d_loc + EPS)
        factors = [jnp.where(total < jnp.inf, inv * jnp.sqrt(q / half + EPS), 0.0) for q in sums]

        def product(at):
            last = sum(jnp.dot(h, weight[l, sp, at], preferred_element_type=F32) for h, sp in hs)
            return sum(f * dg_v[i, :, at] for i, f in enumerate(factors[:-1])) + factors[-1] * last
        return product

    loads["hid"].wait()
    for j in range(2):
        xh[0, j] = hid_v[:, j * half:(j + 1) * half]
    key_lane = lax.broadcasted_iota(jnp.int32, (cells, kl), 1)
    key_row = lax.broadcasted_iota(jnp.int32, (cells, kl), 0)
    group_row = lax.broadcasted_iota(jnp.int32, (16, 1), 0) // heads
    per_group = 16 // heads

    def prepare_rel(l):
        pr = lax.broadcasted_iota(jnp.int32, (kl, kl), 0)
        pc = lax.broadcasted_iota(jnp.int32, (kl, kl), 1)
        flip = (pc == (seq - 1 - pr // heads) * heads + lax.rem(pr, heads)).astype(F32).astype(BF16)
        relf_v[l] = jnp.dot(flip, rel_v[l], preferred_element_type=F32).astype(BF16)
        first = rel_v[l, 0:16].astype(F32)
        for h in range(heads):
            r0_v[l, pl.ds(h, rb, stride=heads), :] = jnp.broadcast_to(first[h:h + 1], (rb, hd))

    def merge(l, new, tile_s, cache):
        for i in range(per_group):
            for h in range(heads):
                tile_s[pl.ds(i * heads + h, rb, stride=16), :] = new[:, h * hd:(h + 1) * hd]
        for b in range(rb):
            tile = tile_s[16 * b:16 * b + 16].astype(BF16)
            at = lent_s[16 * b:16 * b + 16].astype(BF16)
            full = jnp.broadcast_to(tile[None], (kl // 16, 16, hd)).reshape(kl, hd)
            where_at = jnp.broadcast_to(at[None], (kl // 16, 16, hd)).reshape(kl, hd)
            cache[l, b] = jnp.where(pos_v[...] == where_at, full, cache[l, b])

    def prepare_lengths():
        pos_v[...] = (lax.broadcasted_iota(jnp.int32, (kl, hd), 0) // heads).astype(F32).astype(BF16)
        index = my * rb + lax.broadcasted_iota(jnp.int32, (16 * rb, rows), 0) // 16
        lent_s[...] = jnp.broadcast_to(to_column(len_v[...].astype(F32), index), (16 * rb, hd))

    def early_relayout(l, j):
        loads["w", l, j].wait()
        relayout(l, j)

    fills = {}
    if layers > 1:
        fills = {"q": lambda l: early_relayout(l, 0), "up": lambda l: early_relayout(l, 1), "rs": lambda l: early_relayout(l, 2), "rs2": prepare_rel}

    def fill_for(name, l):
        return None if l >= layers or name not in fills else (lambda: fills[name](l))

    for l in range(layers):
        p = 2 * l
        def send_qkv(j):
            for d in y_order:
                peer = lax.rem(my + d, ny)
                rows_at = pl.multiple_of(peer * rb, rb)
                send(qkv_tx.at[l, j, pl.ds(rows_at, rb)], qkv_rx.at[l, my, j], qkv_ss.at[l, j, peer], qkv_rs.at[l, j, my], {"y": peer})

        if l == 0:
            loads["na"].wait()
            norm_stage(p, p, na_v[l:l + 1])
            for j in range(3):
                early_relayout(0, j)
                qkv_tx[l, j] = jnp.dot(h_v[...], wqkv_v[l, :, j * hh:(j + 1) * hh], preferred_element_type=F32).astype(BF16)
                if j == 1:
                    pl.semaphore_wait(barrier, ny - 1 + chips)
                    send_sums(p)
                    send_qkv(0)
                if j:
                    send_qkv(j)
        else:
            product = gather_matmul(p, p - 1, na_v, l, wqkv_v, 3 * hh)
            for j in range(3):
                qkv_tx[l, j] = product(slice(j * hh, (j + 1) * hh)).astype(BF16)
                send_qkv(j)
        own_at = pl.multiple_of(my * rb, rb)
        for j in range(3):
            qkv_rx[l, my, j] = qkv_tx[l, j, pl.ds(own_at, rb), :]
        if l == 0:
            for name in ("len", "rel", "bu", "bw", "nm"):
                loads[name].wait()
            prepare_rel(0)
        loads["k", l].wait()
        loads["v", l].wait()
        lens_row = len_v[...].astype(F32)
        want = my * rb + lax.broadcasted_iota(jnp.int32, (cells, rows), 0) // heads
        lens = to_column(lens_row, want).astype(jnp.int32)
        ratios = ratio_rows(2 * l)
        want16 = my * rb + lax.broadcasted_iota(jnp.int32, (rb, 128), 0)
        cols = [to_column(r, want16) for r in ratios]

        def gathered(j):
            for d in y_order:
                src = lax.rem(my + d, ny)
                recv(qkv_rx.at[l, src, j], qkv_ss.at[l, j, src], qkv_rs.at[l, j, src], {"y": src})
            tot = qkv_rx[l, 0, j].astype(F32) * cols[0]
            for s in range(1, ny):
                tot = tot + qkv_rx[l, s, j].astype(F32) * cols[s]
            return tot.astype(BF16).astype(F32)

        q = gathered(0)
        for h in range(heads):
            qh = q[:, h * hd:(h + 1) * hd]
            a_s[pl.ds(h, rb, stride=heads), :] = qh + bu_v[l, h:h + 1].astype(F32)
            c_s[pl.ds(h, rb, stride=heads), :] = qh + bw_v[l, h:h + 1].astype(F32)
        a = a_s[...].astype(BF16)
        c = c_s[...].astype(BF16)
        rel = lax.dot_general(c, relf_v[l], (((1,), (1,)), ((), ())), preferred_element_type=F32)
        shift = seq - 1 - lens
        unit = 1
        while unit < seq:
            digit = lax.rem(shift // unit, 4)
            rolled = rel
            for m in range(1, 4):
                if m * unit < seq:
                    rolled = jnp.where(digit == m, pltpu.roll(rel, kl - m * unit * heads, 1), rolled)
            rel = rolled
            unit *= 4
        score_parts = []
        for g in range(cells // 16):
            ag = a[16 * g:16 * g + 16]
            sg = None
            for i in range(per_group):
                o = lax.dot_general(ag, kc_v[l, g * per_group + i], (((1,), (1,)), ((), ())), preferred_element_type=F32)
                sg = o if sg is None else jnp.where(group_row == i, o, sg)
            score_parts.append(sg)
        scores = jnp.concatenate(score_parts, axis=0)
        k = gathered(1)
        v = gathered(2)
        for h in range(heads):
            k_s[pl.ds(h, rb, stride=heads), :] = k[:, h * hd:(h + 1) * hd]
            v_s[pl.ds(h, rb, stride=heads), :] = v[:, h * hd:(h + 1) * hd]
        kn = k_s[...]
        vn = v_s[...]
        scale = hd ** -0.5
        s_new = (jnp.sum(a.astype(F32) * kn, axis=1, keepdims=True) + jnp.sum(c.astype(F32) * r0_v[l], axis=1, keepdims=True)) * scale
        valid = (lax.rem(key_lane, heads) == lax.rem(key_row, heads)) & (key_lane // heads < lens)
        scores = jnp.where(valid, (scores + rel) * scale, -jnp.inf)
        top = jnp.maximum(jnp.max(scores, axis=1, keepdims=True), s_new)
        e = jnp.exp(scores - top)
        e_new = jnp.exp(s_new - top)
        inv_den = 1.0 / (jnp.sum(e, axis=1, keepdims=True) + e_new)
        prob = (e * inv_den).astype(BF16)
        p_new = (e_new * inv_den).astype(BF16).astype(F32)
        ctx_parts = []
        for g in range(cells // 16):
            pg = prob[16 * g:16 * g + 16]
            cg = None
            for i in range(0, per_group, 2):
                b = g * per_group + i
                values = jnp.concatenate([vc_v[l, b], vc_v[l, b + 1]], axis=1)
                o = jnp.dot(pg, values, preferred_element_type=F32)
                cg = o[:, :hd] if cg is None else jnp.where(group_row == i, o[:, :hd], cg)
                cg = jnp.where(group_row == i + 1, o[:, hd:], cg)
            ctx_parts.append(cg)
        ctx_s[...] = jnp.concatenate(ctx_parts, axis=0) + p_new * vn
        for h in range(heads):
            ctx_all[l, my, :, h * hd:(h + 1) * hd] = ctx_s[pl.ds(h, rb, stride=heads), :].astype(BF16)
        for d in y_order:
            peer = lax.rem(my + d, ny)
            send(ctx_all.at[l, my], ctx_all.at[l, my], ctx_ss.at[l, peer], ctx_rs.at[l, my], {"y": peer})
        if l == 0:
            prepare_lengths()
        if fill_for("q", l + 1) is not None:
            fills["q"](l + 1)
        merge(l, k, kt_s, kc_v)
        merge(l, v, vt_s, vc_v)
        loads["o", l].wait()
        for d in reversed(y_order):
            src = lax.rem(my + d, ny)
            recv(ctx_all.at[l, src], ctx_ss.at[l, src], ctx_rs.at[l, src], {"y": src})
        ctx = jnp.concatenate([ctx_all[l, s] for s in range(ny)], axis=0)
        x_reduce(p, lambda at: jnp.dot(ctx, wo_v[l, :, at], preferred_element_type=F32), fill_for("rs", l + 1))
        p = 2 * l + 1
        loads["up", l].wait()
        product = gather_matmul(p, p - 1, nm_v, l, wup_v, ff_loc)
        def up_blocks(w, dst, to):
            block = product(pl.ds(pl.multiple_of(dst * fb + w * fw, fw), fw)).astype(BF16)
            for i in range(2):
                to[l, 2 * w + i, dst] = block[:, i * fh:(i + 1) * fh]

        for w in range(2):
            for d in y_order:
                up_blocks(w, lax.rem(my + d, ny), up_tx)
        for w in range(2):
            for hf in (2 * w, 2 * w + 1):
                for d in y_order:
                    dst = lax.rem(my + d, ny)
                    send(up_tx.at[l, hf, dst], up_rx.at[l, hf, my], up_ss.at[l, hf, dst], up_rs.at[l, hf, my], {"y": dst})
        for w in range(2):
            up_blocks(w, my, up_rx)
        if fill_for("up", l + 1) is not None:
            fills["up"](l + 1)
        ratios = ratio_rows(p)
        cols = [to_column(r, rown) for r in ratios]
        loads["dn", l].wait()
        for hf in range(4):
            for d in reversed(y_order):
                src = lax.rem(my + d, ny)
                recv(up_rx.at[l, hf, src], up_ss.at[l, hf, src], up_rs.at[l, hf, src], {"y": src})
            tot = up_rx[l, hf, 0].astype(F32) * cols[0]
            for s in range(1, ny):
                tot = tot + up_rx[l, hf, s].astype(F32) * cols[s]
            act[l, hf, my] = jax.nn.gelu(tot.astype(BF16).astype(F32), approximate=True).astype(BF16)
            for d in y_order:
                peer = lax.rem(my + d, ny)
                send(act.at[l, hf, my], act.at[l, hf, my], act_ss.at[l, hf, peer], act_rs.at[l, hf, my], {"y": peer})

        def down(w, src, at=slice(None)):
            pieces = jnp.concatenate([act[l, 2 * w, src], act[l, 2 * w + 1, src]], axis=1)
            return jnp.dot(pieces, wdn_v[l, pl.ds(pl.multiple_of(src * fb + w * fw, fw), fw), at], preferred_element_type=F32)

        acc_v[...] = down(0, my) + down(1, my)
        steps = [(w, d) for w in range(2) for d in down_order]
        for w, d in steps:
            src = lax.rem(my + d, ny)
            for hf in (2 * w, 2 * w + 1):
                recv(act.at[l, hf, src], act_ss.at[l, hf, src], act_rs.at[l, hf, src], {"y": src})
            if (w, d) != steps[-1]:
                acc_v[...] += down(w, src)
        x_reduce(p, lambda at: acc_v[:, at] + down(w, src, at), fill_for("rs2", l + 1))
    recv_half(2 * layers - 1)

    last = 2 * layers
    for j in range(2):
        hid_out[:, j * half:(j + 1) * half] = xh[last, j]
    for c in sends:
        c.wait_send()


def write_kernel(hid_in, kc_in, vc_in, hid_out, kc_out, vc_out, sem):
    copies = [pltpu.make_async_copy(hid_in, hid_out, sem.at[0])]
    layers, rb = kc_in.shape[:2]
    half = rb // 2
    for src, dst in ((kc_in, kc_out), (vc_in, vc_out)):
        for l in range(layers):
            for b in range(0, rb, half):
                copies.append(pltpu.make_async_copy(src.at[l, pl.ds(b, half)], dst.at[l, pl.ds(b, half)], sem.at[len(copies)]))
    for c in copies:
        c.start()
    for c in copies:
        c.wait()


def solution(mesh):
    ny = mesh.shape["y"]
    nx = mesh.shape["x"]
    cache_spec = P(None, ("rep", "y"), None, "x", None)
    row_spec = P("rep", "y")
    proj_spec = P(None, "y", "x", None)
    head_spec = P(None, "x", None)
    in_specs = (row_spec, P("rep"), cache_spec, cache_spec, P(None, None, "x", None), P(None, "y"),
                proj_spec, proj_spec, proj_spec, head_spec, head_spec, P(None, "x", None, "y"),
                P(None, "y"), P(None, "y", "x"), P(None, "x", "y"))
    out_specs = (row_spec, cache_spec, cache_spec)

    def local_step(hidden, lengths, k_cache, v_cache, rel_table, norm_attn, w_q, w_k, w_v, bias_content, bias_pos, w_out, norm_mlp, w_up, w_down):
        layers, rb, seq, heads, hd = k_cache.shape
        rows, d_loc = hidden.shape
        ff_loc = w_up.shape[2]
        hh = heads * hd
        cells = rb * heads
        kl = seq * heads
        half = d_loc // 2
        fb = ff_loc // ny
        dims = (layers, ny, nx, rows, heads, hd, seq, d_loc, ff_loc)
        any_spec = pl.BlockSpec(memory_space=pl.ANY)
        vmem = pltpu.VMEM
        dma = pltpu.SemaphoreType.DMA
        scratch = [
            vmem((rows, d_loc), BF16), vmem((1, rows), jnp.int32),
            vmem((layers, kl, hd), BF16), vmem((layers, d_loc), BF16), vmem((layers, d_loc), BF16),
            vmem((layers, heads, hd), BF16), vmem((layers, heads, hd), BF16),
            vmem((layers, 3, d_loc * heads, hd), BF16), vmem((layers, d_loc, 3 * hh), BF16),
            vmem((layers, hh, d_loc), BF16), vmem((layers, d_loc, ff_loc), BF16), vmem((layers, ff_loc, d_loc), BF16),
            vmem((128 * heads, hd), F32), vmem((layers, kl, hd), BF16), vmem((layers, cells, hd), F32), vmem((rows, d_loc), BF16),
            vmem((cells, hd), F32), vmem((cells, hd), F32), vmem((cells, hd), F32), vmem((cells, hd), F32), vmem((cells, hd), F32),
            vmem((rows, d_loc), F32), vmem((kl, hd), BF16), vmem((16 * rb, hd), F32), vmem((16 * rb, hd), F32), vmem((16 * rb, hd), F32),
            vmem((1, rows, max(ff_loc, 3 * hh)), F32),
            vmem((2 * layers, ny, 8, 128), F32),
            vmem((layers, 3, rows, hh), BF16), vmem((layers, ny, 3, rb, hh), BF16), vmem((layers, ny, rb, hh), BF16),
            vmem((2 * layers, rows, half), BF16), vmem((2 * layers, rows, half), BF16), vmem((2 * layers, nx // 2, rows, half), BF16), vmem((2 * layers + 1, 2, rows, half), BF16),
            vmem((layers, 4, ny, rows, fb // 4), BF16), vmem((layers, 4, ny, rows, fb // 4), BF16), vmem((layers, 4, ny, rows, fb // 4), BF16),
            dma((7 + 8 * layers,)),
            dma((2 * layers, ny)), dma((2 * layers, ny)), dma((layers, 3, ny)), dma((layers, 3, ny)),
            dma((layers, ny)), dma((layers, ny)), dma((2 * layers,)), dma((2 * layers,)), dma((2 * layers, nx // 2)), dma((2 * layers, nx // 2)),
            dma((2 * layers,)), dma((2 * layers,)), dma((layers, 4, ny)), dma((layers, 4, ny)), dma((layers, 4, ny)), dma((layers, 4, ny)),
        ]
        cache_dims = (layers, rb, kl, hd)
        vmem_spec = pl.BlockSpec(memory_space=vmem)
        hid, k_new, v_new = pl.pallas_call(
            functools.partial(step_kernel, dims),
            out_shape=(vmem((rows, d_loc), BF16), vmem(cache_dims, BF16), vmem(cache_dims, BF16)),
            in_specs=[any_spec] * 15,
            out_specs=(vmem_spec,) * 3,
            scratch_shapes=scratch,
            compiler_params=pltpu.CompilerParams(collective_id=0, has_side_effects=True, vmem_limit_bytes=46 * 1024 * 1024),
            name="decode_step",
        )(hidden, lengths.reshape(1, rows), k_cache.reshape(layers, rb, kl, hd), v_cache.reshape(layers, rb, kl, hd),
          rel_table.reshape(layers, kl, hd), norm_attn,
          w_q.reshape(layers, d_loc * heads, hd), w_k.reshape(layers, d_loc * heads, hd), w_v.reshape(layers, d_loc * heads, hd),
          bias_content, bias_pos, w_out.reshape(layers, hh, d_loc), norm_mlp, w_up, w_down)

        flat = jax.ShapeDtypeStruct(cache_dims, BF16)
        hid, k_new, v_new = pl.pallas_call(
            write_kernel,
            out_shape=(jax.ShapeDtypeStruct((rows, d_loc), BF16), flat, flat),
            in_specs=[vmem_spec] * 3,
            out_specs=(any_spec,) * 3,
            scratch_shapes=[dma((1 + 4 * layers,))],
            compiler_params=pltpu.CompilerParams(vmem_limit_bytes=2 * 1024 * 1024),
            name="cache_write",
        )(hid, k_new, v_new)
        return hid, k_new.reshape(k_cache.shape), v_new.reshape(v_cache.shape)

    return jax.shard_map(local_step, mesh=mesh, in_specs=in_specs, out_specs=out_specs, check_vma=False)
```
